8 devices in a mesh: rep: 2 (over z, y), grp: 4 (over x, core).
Axes of the slice: x: 2, y: 2, z: 1, core: 2. Of those that a mesh axis runs over, the one named last changes fastest.
Arguments:
- x_in: bfloat16 [512, 2048], P(('rep', 'grp')), parts along dimension 0
- seq_len: int32 [512], P(('rep', 'grp')), parts along dimension 0
- k_cache: bfloat16 [512, 256, 2, 128], P(('rep', 'grp')), parts along dimension 0
- v_cache: bfloat16 [512, 256, 2, 128], P(('rep', 'grp')), parts along dimension 0
- gamma_attn: bfloat16 [2048], replicated
- w_qkv: bfloat16 [2048, 2560], replicated
- b_qkv: bfloat16 [2560], replicated
- w_proj: bfloat16 [2048, 2048], replicated
- gamma_mlp: bfloat16 [2048], replicated
- w_in: bfloat16 [2, 11008, 2048], P(None, 'grp')
- w_out: bfloat16 [11008, 2048], P('grp')
Outputs:
- output 1: bfloat16 [512, 2048], P(('rep', 'grp')), parts along dimension 0
- output 2: bfloat16 [512, 256, 2, 128], P(('rep', 'grp')), parts along dimension 0
- output 3: bfloat16 [512, 256, 2, 128], P(('rep', 'grp')), parts along dimension 0
There are 2 independent parts. The reference program is written for one: setup_inputs(seed, part) draws one part's arguments, and reference() takes and returns one part's arrays. A program takes and returns all parts, laid end to end along the dimension named above; an argument that names none is the same for every part.
All inputs are finite; a program needn't handle non-finite values.
Results may differ from the reference program's by a relative error of at most 0.00743079.
Values are sent between devices in bfloat16 or wider.
A program may use at most 1 GiB of HBM per device.

```python
import jax
import jax.numpy as jnp
from jax import lax

HIDDEN = 2048
HEADS = 16
KV_HEADS = 2
HEAD = 128
FFN = 11008
LMAX = 256
BATCH = 256
ROPE_BASE = 10000
QKV_WIDTH = (HEADS + 2 * KV_HEADS) * HEAD
ROT_DIM = HEAD // 2
EPS = 1e-5


def setup_inputs(seed: int = 0, part: int = 0) -> dict:
    keys = jax.random.split(jax.random.key(seed), 10)
    gamma_attn = (1.0 + 0.3 * jax.random.normal(keys[0], (HIDDEN,), jnp.float32)).astype(jnp.bfloat16)
    w_qkv = (jax.random.normal(keys[1], (HIDDEN, QKV_WIDTH), jnp.float32) * HIDDEN ** -0.5).astype(jnp.bfloat16)
    b_qkv = (0.5 * jax.random.normal(keys[2], (QKV_WIDTH,), jnp.float32)).astype(jnp.bfloat16)
    w_proj = (jax.random.normal(keys[3], (HEADS * HEAD, HIDDEN), jnp.float32) * (HEADS * HEAD) ** -0.5).astype(jnp.bfloat16)
    gamma_mlp = (1.0 + 0.3 * jax.random.normal(keys[4], (HIDDEN,), jnp.float32)).astype(jnp.bfloat16)
    w_in = (jax.random.normal(keys[5], (2, FFN, HIDDEN), jnp.float32) * HIDDEN ** -0.5).astype(jnp.bfloat16)
    w_out = (jax.random.normal(keys[6], (FFN, HIDDEN), jnp.float32) * FFN ** -0.5).astype(jnp.bfloat16)
    x_in = jax.random.normal(jax.random.fold_in(keys[7], part), (BATCH, HIDDEN), jnp.float32).astype(jnp.bfloat16)
    seq_len = jax.random.randint(jax.random.fold_in(keys[8], part), (BATCH,), 1, LMAX, dtype=jnp.int32)
    seq_len = seq_len.at[0].set(LMAX - 1).at[BATCH - 1].set(1)
    cache_keys = jax.random.split(jax.random.fold_in(keys[9], part), 3)
    cache_shape = (BATCH, LMAX, KV_HEADS, HEAD)
    k_cache = (2.0 * jax.random.normal(cache_keys[0], cache_shape, jnp.float32)).astype(jnp.bfloat16)
    drift = jnp.cumsum(jax.random.normal(cache_keys[1], cache_shape, jnp.float32), axis=1) * LMAX ** -0.5
    v_cache = (drift + jax.random.normal(cache_keys[2], cache_shape, jnp.float32)).astype(jnp.bfloat16)
    return {'x_in': x_in, 'seq_len': seq_len, 'k_cache': k_cache, 'v_cache': v_cache,
            'gamma_attn': gamma_attn, 'w_qkv': w_qkv, 'b_qkv': b_qkv, 'w_proj': w_proj,
            'gamma_mlp': gamma_mlp, 'w_in': w_in, 'w_out': w_out}


def rms_norm(vals, gain):
    mean_sq = jnp.mean(vals * vals, axis=-1, keepdims=True)
    return (vals * lax.rsqrt(mean_sq + EPS) * gain.astype(jnp.float32)).astype(jnp.bfloat16)


def rotary(vals, positions):
    inv_freq = ROPE_BASE ** (-jnp.arange(0, ROT_DIM, 2, dtype=jnp.float32) / ROT_DIM)
    angles = positions.astype(jnp.float32)[:, None] * inv_freq[None, :]
    cosine = jnp.cos(angles)[:, None, :]
    sine = jnp.sin(angles)[:, None, :]
    pairs = vals[..., :ROT_DIM].reshape(vals.shape[:-1] + (ROT_DIM // 2, 2))
    even_part = pairs[..., 0]
    odd_part = pairs[..., 1]
    rotated = jnp.stack([even_part * cosine - odd_part * sine, odd_part * cosine + even_part * sine], axis=-1)
    return jnp.concatenate([rotated.reshape(vals.shape[:-1] + (ROT_DIM,)), vals[..., ROT_DIM:]], axis=-1)


def reference(x_in, seq_len, k_cache, v_cache, gamma_attn, w_qkv, b_qkv, w_proj, gamma_mlp, w_in, w_out):
    x_f32 = x_in.astype(jnp.float32)
    normed = rms_norm(x_f32, gamma_attn)
    qkv_proj = jnp.dot(normed, w_qkv, preferred_element_type=jnp.float32) + b_qkv.astype(jnp.float32)
    q_width = HEADS * HEAD
    kv_width = KV_HEADS * HEAD
    query_rot = rotary(qkv_proj[:, :q_width].reshape(BATCH, HEADS, HEAD), seq_len).astype(jnp.bfloat16)
    key_new = rotary(qkv_proj[:, q_width:q_width + kv_width].reshape(BATCH, KV_HEADS, HEAD), seq_len).astype(jnp.bfloat16)
    value_new = qkv_proj[:, q_width + kv_width:].reshape(BATCH, KV_HEADS, HEAD).astype(jnp.bfloat16)
    positions = jnp.arange(LMAX, dtype=jnp.int32)
    at_len = (positions[None, :] == seq_len[:, None])[:, :, None, None]
    k_out = jnp.where(at_len, key_new[:, None], k_cache)
    v_out = jnp.where(at_len, value_new[:, None], v_cache)

    def one_seq(seq_args):
        q_row, k_row, v_row, length = seq_args
        q_grouped = q_row.reshape(KV_HEADS, HEADS // KV_HEADS, HEAD).astype(jnp.float32)
        attn_scores = jnp.einsum('gqd,lgd->gql', q_grouped, k_row.astype(jnp.float32)) * HEAD ** -0.5
        attn_scores = jnp.where((positions <= length)[None, None, :], attn_scores, -jnp.inf)
        attn_probs = jax.nn.softmax(attn_scores, axis=-1).astype(jnp.bfloat16)
        context = jnp.einsum('gql,lgd->gqd', attn_probs.astype(jnp.float32), v_row.astype(jnp.float32))
        return context.reshape(HEADS * HEAD).astype(jnp.bfloat16)

    context = lax.map(one_seq, (query_rot, k_out, v_out, seq_len))
    hidden = x_f32 + jnp.dot(context, w_proj, preferred_element_type=jnp.float32)
    mlp_in = rms_norm(hidden, gamma_mlp)
    gate_up = jnp.dot(mlp_in, w_in.reshape(2 * FFN, HIDDEN).T, preferred_element_type=jnp.float32)
    swiglu = (jax.nn.silu(gate_up[:, :FFN]) * gate_up[:, FFN:]).astype(jnp.bfloat16)
    mlp_out = jnp.dot(swiglu, w_out, preferred_element_type=jnp.float32)
    layer_out = (hidden + mlp_out).astype(jnp.bfloat16)
    return (layer_out, k_out, v_out)
```

```python
import jax
import jax.numpy as jnp
from jax import lax
from jax.experimental import pallas as pl
from jax.experimental.pallas import tpu as pltpu
from jax.sharding import PartitionSpec as P

HEAD_DIM = 128
ROPE_BASE = 10000.0
EPS = 1e-5
HIDDEN = 2048
HEADS = 16
KV = 2
ROWS = 64
LMAX = 256
FLAT = LMAX * KV
FFN_LOC = 2752
QKV_CHUNK = 512
N_QKV = 5
PROJ_CHUNK = 512
N_PROJ = 4
SEQ_CHUNK = 8
N_SEQ = ROWS // SEQ_CHUNK
SUB = 4
F_CHUNK = 256
N_F = 11
D_CHUNK = 256
N_D = HIDDEN // D_CHUNK
AG_PIECES = 4
AG_ROWS = ROWS // AG_PIECES
LAG = 6
F32 = jnp.float32
BF16 = jnp.bfloat16


def attn_kernel(len_ref, x_ref, cos_ref, sin_ref, ga_ref, gm_ref, b_ref, wqkv_hbm, k_hbm, v_hbm, wproj_hbm,
                h_ref, m_ref, kout_hbm, vout_hbm,
                wq_buf, wp_buf, k_buf, v_buf, q_scr, kn_scr, vn_scr, ctx_scr, act_buf,
                wq_sem, wp_sem, k_sem, v_sem, ko_sem, vo_sem):
    def wq_copy(c):
        return pltpu.make_async_copy(wqkv_hbm.at[:, pl.ds(c * QKV_CHUNK, QKV_CHUNK)], wq_buf.at[c], wq_sem.at[c])

    def wp_copy(c):
        return pltpu.make_async_copy(wproj_hbm.at[:, pl.ds(c * PROJ_CHUNK, PROJ_CHUNK)], wp_buf.at[c], wp_sem.at[c])

    def k_copy(i):
        rows = pl.ds(i * SEQ_CHUNK, SEQ_CHUNK)
        return pltpu.make_async_copy(k_hbm.at[rows], k_buf.at[rows], k_sem.at[i])

    def v_copy(i):
        rows = pl.ds(i * SEQ_CHUNK, SEQ_CHUNK)
        return pltpu.make_async_copy(v_hbm.at[rows], v_buf.at[rows], v_sem.at[i])

    def ko_copy(i):
        rows = pl.ds(i * SEQ_CHUNK, SEQ_CHUNK)
        return pltpu.make_async_copy(k_buf.at[rows], kout_hbm.at[rows], ko_sem.at[i])

    def vo_copy(i):
        rows = pl.ds(i * SEQ_CHUNK, SEQ_CHUNK)
        return pltpu.make_async_copy(v_buf.at[rows], vout_hbm.at[rows], vo_sem.at[i])

    for c in range(N_QKV):
        wq_copy(c).start()
    for i in range(N_SEQ):
        k_copy(i).start()
        v_copy(i).start()
    for c in range(N_PROJ):
        wp_copy(c).start()

    x = x_ref[...].astype(F32)
    inv = lax.rsqrt(jnp.mean(x * x, axis=-1, keepdims=True) + EPS)
    act_buf[...] = (x * inv * ga_ref[...]).astype(BF16)
    normed = act_buf[...]
    cosine = cos_ref[...]
    sine = sin_ref[...]
    even = (lax.broadcasted_iota(jnp.int32, (ROWS, HEAD_DIM), 1) % 2) == 0

    def rotate(v):
        swapped = jnp.where(even, pltpu.roll(v, HEAD_DIM - 1, 1), pltpu.roll(v, 1, 1))
        return v * cosine + swapped * sine

    for c in range(N_QKV):
        wq_copy(c).wait()
        cols = pl.ds(c * QKV_CHUNK, QKV_CHUNK)
        acc = jnp.dot(normed, wq_buf[c], preferred_element_type=F32) + b_ref[:, cols]
        for t in range(QKV_CHUNK // HEAD_DIM):
            head = c * (QKV_CHUNK // HEAD_DIM) + t
            part = acc[:, t * HEAD_DIM:(t + 1) * HEAD_DIM]
            if head < HEADS:
                q_scr[pl.ds(head, ROWS, stride=HEADS), :] = rotate(part)
            elif head < HEADS + KV:
                kn_scr[head - HEADS] = rotate(part)
            else:
                vn_scr[head - HEADS - KV] = part

    row16 = lax.broadcasted_iota(jnp.int32, (16, HEAD_DIM), 0)
    col = lax.broadcasted_iota(jnp.int32, (HEADS, FLAT), 1)
    head_row = lax.broadcasted_iota(jnp.int32, (HEADS, FLAT), 0)
    pos = jnp.where((col % KV) == (head_row // (HEADS // KV)), col // KV, 2 * LMAX)

    def chunk_body(i, carry):
        k_copy(i).wait()
        v_copy(i).wait()
        for u in range(SEQ_CHUNK):
            b = i * SEQ_CHUNK + u
            ln = len_ref[b]
            base = pl.multiple_of((ln // 8) * 16, 16)
            hit = (row16 // 2) == (ln % 8)
            for buf, new in ((k_buf, kn_scr), (v_buf, vn_scr)):
                fresh = jnp.where(row16 % 2 == 0, new[0, pl.ds(b, 1), :], new[1, pl.ds(b, 1), :])
                old = buf[b, pl.ds(base, 16), :].astype(F32)
                buf[b, pl.ds(base, 16), :] = jnp.where(hit, fresh, old).astype(BF16)
        for s0 in range(0, SEQ_CHUNK, SUB):
            probs = []
            for u in range(s0, s0 + SUB):
                b = i * SEQ_CHUNK + u
                q = q_scr[pl.ds(pl.multiple_of(b * HEADS, HEADS), HEADS), :].astype(BF16)
                s = lax.dot_general(q, k_buf[b], (((1,), (1,)), ((), ())), preferred_element_type=F32)
                s = jnp.where(pos <= len_ref[b], s * (HEAD_DIM ** -0.5), -jnp.inf)
                e = jnp.exp(s - jnp.max(s, axis=1, keepdims=True))
                probs.append((e / jnp.sum(e, axis=1, keepdims=True)).astype(BF16))
            for u in range(s0, s0 + SUB):
                b = i * SEQ_CHUNK + u
                ctx_scr[pl.ds(pl.multiple_of(b * HEADS, HEADS), HEADS), :] = jnp.dot(
                    probs[u - s0], v_buf[b], preferred_element_type=F32)
        ko_copy(i).start()
        vo_copy(i).start()
        return carry

    lax.fori_loop(0, N_SEQ, chunk_body, 0)

    for h in range(HEADS):
        act_buf[:, h * HEAD_DIM:(h + 1) * HEAD_DIM] = ctx_scr[pl.ds(h, ROWS, stride=HEADS), :].astype(BF16)
    ctx = act_buf[...]
    total = jnp.zeros((ROWS, 1), F32)
    for c in range(N_PROJ):
        wp_copy(c).wait()
        cols = slice(c * PROJ_CHUNK, (c + 1) * PROJ_CHUNK)
        hid = x_ref[:, cols].astype(F32) + jnp.dot(ctx, wp_buf[c], preferred_element_type=F32)
        h_ref[:, cols] = hid
        total = total + jnp.sum(hid * hid, axis=-1, keepdims=True)
    inv2 = lax.rsqrt(total * (1.0 / HIDDEN) + EPS)
    for c in range(N_PROJ):
        cols = slice(c * PROJ_CHUNK, (c + 1) * PROJ_CHUNK)
        m_ref[:, cols] = (h_ref[:, cols] * inv2 * gm_ref[:, cols]).astype(BF16)
    for i in range(N_SEQ):
        ko_copy(i).wait()
        vo_copy(i).wait()


def attention(lens, x, cosine, sine, ga, gm, bias, w_qkv, k_flat, v_flat, w_proj):
    vmem = pl.BlockSpec(memory_space=pltpu.VMEM)
    hbm = pl.BlockSpec(memory_space=pl.ANY)
    smem = pl.BlockSpec(memory_space=pltpu.SMEM)
    dma = pltpu.SemaphoreType.DMA
    return pl.pallas_call(
        attn_kernel,
        out_shape=(jax.ShapeDtypeStruct((ROWS, HIDDEN), F32), jax.ShapeDtypeStruct((ROWS, HIDDEN), BF16),
                   jax.ShapeDtypeStruct(k_flat.shape, BF16), jax.ShapeDtypeStruct(v_flat.shape, BF16)),
        in_specs=[smem] + [vmem] * 6 + [hbm] * 4,
        out_specs=(vmem, vmem, hbm, hbm),
        scratch_shapes=[
            pltpu.VMEM((N_QKV, HIDDEN, QKV_CHUNK), BF16),
            pltpu.VMEM((N_PROJ, HIDDEN, PROJ_CHUNK), BF16),
            pltpu.VMEM((ROWS, FLAT, HEAD_DIM), BF16),
            pltpu.VMEM((ROWS, FLAT, HEAD_DIM), BF16),
            pltpu.VMEM((ROWS * HEADS, HEAD_DIM), F32),
            pltpu.VMEM((KV, ROWS, HEAD_DIM), F32),
            pltpu.VMEM((KV, ROWS, HEAD_DIM), F32),
            pltpu.VMEM((ROWS * HEADS, HEAD_DIM), F32),
            pltpu.VMEM((ROWS, HIDDEN), BF16),
            dma((N_QKV,)), dma((N_PROJ,)), dma((N_SEQ,)), dma((N_SEQ,)), dma((N_SEQ,)), dma((N_SEQ,)),
        ],
        compiler_params=pltpu.CompilerParams(vmem_limit_bytes=60 * 1024 * 1024),
        name="attn_block",
    )(lens, x, cosine, sine, ga, gm, bias, w_qkv, k_flat, v_flat, w_proj)


def mlp_kernel(m_ref, h_ref, win_hbm, wout_hbm, y_ref,
               rows_buf, win_buf, wout_buf, g_buf, pair_send, pair_recv, near_send, near_recv, far_keep, far_send, far_recv,
               own_acc, win_sem, wout_sem, agx_s, agx_r, agp_s, agp_r, agr_s, agr_r,
               ps_s, ps_r, ns_s, ns_r, fs_s, fs_r):
    me = lax.axis_index('grp')
    partner = me + 1 - 2 * (me % 2)
    cross = (me + 2) % 4

    def win_copy(i, part, width):
        rows = pl.ds(i * F_CHUNK, width)
        return pltpu.make_async_copy(win_hbm.at[part, rows], win_buf.at[part, rows], win_sem.at[part, i])

    def wout_copy(j):
        cols = pl.ds(j * D_CHUNK, D_CHUNK)
        return pltpu.make_async_copy(wout_hbm.at[:, cols], wout_buf.at[:, cols], wout_sem.at[j])

    tail = FFN_LOC - (N_F - 1) * F_CHUNK
    widths = [F_CHUNK] * (N_F - 1) + [tail]
    for i in range(N_F):
        for part in range(2):
            win_copy(i, part, widths[i]).start()
    for j in range(N_D):
        wout_copy(j).start()

    barrier = pltpu.get_barrier_semaphore()
    for peer in (partner, cross):
        pl.semaphore_signal(barrier, inc=1, device_id={'grp': peer}, device_id_type=pl.DeviceIdType.MESH)
    pl.semaphore_wait(barrier, 2)

    def send(src, dst, ssem, rsem, peer):
        return pltpu.make_async_remote_copy(src_ref=src, dst_ref=dst, send_sem=ssem, recv_sem=rsem,
                                            device_id={'grp': peer}, device_id_type=pl.DeviceIdType.MESH)

    cross_copies = [send(m_ref.at[pl.ds(p * AG_ROWS, AG_ROWS)], rows_buf.at[pl.ds(2 * ROWS + p * AG_ROWS, AG_ROWS)],
                         agx_s.at[p], agx_r.at[p], cross) for p in range(AG_PIECES)]
    for cp in cross_copies:
        cp.start()
    pair_copy = send(m_ref, rows_buf.at[pl.ds(ROWS, ROWS)], agp_s, agp_r, partner)
    pair_copy.start()
    rows_buf[pl.ds(0, ROWS), :] = m_ref[...]
    relays = []
    for p in range(AG_PIECES):
        cross_copies[p].wait_recv()
        relay = send(rows_buf.at[pl.ds(2 * ROWS + p * AG_ROWS, AG_ROWS)],
                     rows_buf.at[pl.ds(3 * ROWS + p * AG_ROWS, AG_ROWS)], agr_s.at[p], agr_r.at[p], partner)
        relay.start()
        relays.append(relay)
    pair_copy.wait()
    for p in range(AG_PIECES):
        cross_copies[p].wait_send()
        relays[p].wait()

    def ffn_chunk(i, width):
        for part in range(2):
            win_copy(i, part, width).wait()
        fr = pl.ds(pl.multiple_of(i * F_CHUNK, F_CHUNK), width)
        rows = rows_buf[...]
        dims = (((1,), (1,)), ((), ()))
        gate = lax.dot_general(rows, win_buf[0, fr, :], dims, preferred_element_type=F32)
        up = lax.dot_general(rows, win_buf[1, fr, :], dims, preferred_element_type=F32)
        g_buf[:, fr] = (gate * jax.nn.sigmoid(gate) * up).astype(BF16)

    lax.fori_loop(0, N_F - 1, lambda i, c: (ffn_chunk(i, F_CHUNK), c)[1], 0)
    ffn_chunk(N_F - 1, tail)

    pair_copies = [send(pair_send.at[j], pair_recv.at[j], ps_s.at[j], ps_r.at[j], partner) for j in range(N_D)]
    near_copies = [send(near_send.at[j], near_recv.at[j], ns_s.at[j], ns_r.at[j], partner) for j in range(N_D)]
    far_copies = [send(far_send.at[j], far_recv.at[j], fs_s.at[j], fs_r.at[j], cross) for j in range(N_D)]

    for step in range(2 * N_D + 2):
        if 1 <= step <= N_D:
            pair_copies[step - 1].start()
        elif N_D < step <= 2 * N_D:
            near_copies[step - 1 - N_D].start()
        if LAG + 1 <= step <= LAG + N_D:
            far_copies[step - LAG - 1].start()
        if step < N_D:
            wout_copy(step).wait()
            cols = slice(step * D_CHUNK, (step + 1) * D_CHUNK)
            part = jnp.dot(g_buf[2 * ROWS:, :], wout_buf[:, cols], preferred_element_type=F32)
            far_keep[step] = part[:ROWS]
            pair_send[step] = part[ROWS:].astype(BF16)
        elif step < 2 * N_D:
            j = step - N_D
            cols = slice(j * D_CHUNK, (j + 1) * D_CHUNK)
            part = jnp.dot(g_buf[:2 * ROWS, :], wout_buf[:, cols], preferred_element_type=F32)
            own_acc[j] = part[:ROWS] + h_ref[:, cols]
            near_send[j] = part[ROWS:].astype(BF16)
        if LAG <= step < LAG + N_D:
            j = step - LAG
            pair_copies[j].wait_recv()
            far_send[j] = (far_keep[j] + pair_recv[j].astype(F32)).astype(BF16)

    for j in range(N_D):
        cols = slice(j * D_CHUNK, (j + 1) * D_CHUNK)
        near_copies[j].wait_recv()
        far_copies[j].wait_recv()
        y_ref[:, cols] = (own_acc[j] + near_recv[j].astype(F32) + far_recv[j].astype(F32)).astype(BF16)
    for j in range(N_D):
        pair_copies[j].wait_send()
        near_copies[j].wait_send()
        far_copies[j].wait_send()


def mlp(m, h, w_in, w_out):
    vmem = pl.BlockSpec(memory_space=pltpu.VMEM)
    hbm = pl.BlockSpec(memory_space=pl.ANY)
    dma = pltpu.SemaphoreType.DMA
    piece = (N_D, ROWS, D_CHUNK)
    return pl.pallas_call(
        mlp_kernel,
        out_shape=jax.ShapeDtypeStruct((ROWS, HIDDEN), BF16),
        in_specs=[vmem, vmem, hbm, hbm],
        out_specs=vmem,
        scratch_shapes=[
            pltpu.VMEM((4 * ROWS, HIDDEN), BF16),
            pltpu.VMEM((2, FFN_LOC, HIDDEN), BF16),
            pltpu.VMEM((FFN_LOC, HIDDEN), BF16),
            pltpu.VMEM((4 * ROWS, FFN_LOC), BF16),
            pltpu.VMEM(piece, BF16), pltpu.VMEM(piece, BF16),
            pltpu.VMEM(piece, BF16), pltpu.VMEM(piece, BF16),
            pltpu.VMEM(piece, F32), pltpu.VMEM(piece, BF16), pltpu.VMEM(piece, BF16),
            pltpu.VMEM(piece, F32),
            dma((2, N_F)), dma((N_D,)),
            dma((AG_PIECES,)), dma((AG_PIECES,)), dma, dma, dma((AG_PIECES,)), dma((AG_PIECES,)),
            dma((N_D,)), dma((N_D,)), dma((N_D,)), dma((N_D,)), dma((N_D,)), dma((N_D,)),
        ],
        compiler_params=pltpu.CompilerParams(vmem_limit_bytes=60 * 1024 * 1024, collective_id=0, has_side_effects=True),
        name="mlp_block",
    )(m, h, w_in, w_out)


def rope_tables(lens):
    rot = HEAD_DIM // 2
    lane = jnp.arange(HEAD_DIM)
    inv_freq = ROPE_BASE ** (-(2 * (lane // 2)).astype(F32) / rot)
    angles = lens.astype(F32)[:, None] * inv_freq[None, :]
    active = lane[None, :] < rot
    sign = jnp.where(lane % 2 == 0, -1.0, 1.0)[None, :]
    return jnp.where(active, jnp.cos(angles), 1.0), jnp.where(active, jnp.sin(angles) * sign, 0.0)


def solution(mesh):
    row_spec = P(('rep', 'grp'))
    repl_spec = P()

    def local_layer(x_in, seq_len, k_cache, v_cache, gamma_attn, w_qkv, b_qkv, w_proj, gamma_mlp, w_in, w_out):
        cosine, sine = rope_tables(seq_len)
        ga = gamma_attn.astype(F32)[None, :]
        gm = gamma_mlp.astype(F32)[None, :]
        bias = b_qkv.astype(F32)[None, :]
        k_flat = k_cache.reshape(ROWS, FLAT, HEAD_DIM)
        v_flat = v_cache.reshape(ROWS, FLAT, HEAD_DIM)
        h, m, k_out, v_out = attention(seq_len, x_in, cosine, sine, ga, gm, bias, w_qkv, k_flat, v_flat, w_proj)
        layer_out = mlp(m, h, w_in, w_out)
        return layer_out, k_out.reshape(k_cache.shape), v_out.reshape(v_cache.shape)

    return jax.shard_map(local_layer, mesh=mesh,
                         in_specs=(row_spec, row_spec, row_spec, row_spec, repl_spec, repl_spec, repl_spec,
                                   repl_spec, repl_spec, P(None, 'grp', None), P('grp', None)),
                         out_specs=(row_spec, row_spec, row_spec), check_vma=False)
```

```python
import jax
import jax.numpy as jnp
import numpy as np
from jax import lax
from jax.experimental import pallas as pl
from jax.experimental.pallas import tpu as pltpu
from jax.sharding import PartitionSpec as P

HEAD_DIM = 128
ROPE_BASE = 10000.0
EPS = 1e-5
HIDDEN = 2048
HEADS = 16
KV = 2
ROWS = 64
LMAX = 256
FLAT = LMAX * KV
FFN_LOC = 2752
QKV_CHUNK = 512
N_QKV = 5
PROJ_CHUNK = 512
N_PROJ = 4
SEQ_CHUNK = 8
N_SEQ = ROWS // SEQ_CHUNK
SUB = 8
WINDOW = 7
F_CHUNK = 256
N_F = 11
D_CHUNK = 256
N_D = HIDDEN // D_CHUNK
AG_PIECES = 4
AG_ROWS = ROWS // AG_PIECES
LAG = 6
F32 = jnp.float32
BF16 = jnp.bfloat16


def attn_kernel(len_ref, freq_hbm, x_hbm, ga_hbm, gm_hbm, b_hbm, wqkv_hbm, k_hbm, v_hbm, wproj_hbm,
                h_hbm, m_hbm, kout_hbm, vout_hbm,
                freq_ref, x_ref, ga_ref, gm_ref, b_ref, h_ref, m_ref,
                wq_buf, wp_buf, k_buf, v_buf, q_scr, kn_scr, vn_scr, ctx_scr, act_buf,
                small_sem, wq_sem, wp_sem, k_sem, v_sem, ko_sem, vo_sem, out_sem):
    small = [pltpu.make_async_copy(src, dst, small_sem.at[n]) for n, (src, dst) in enumerate(
        ((x_hbm, x_ref), (ga_hbm, ga_ref), (freq_hbm, freq_ref), (b_hbm, b_ref), (gm_hbm, gm_ref)))]

    def wq_copy(c):
        return pltpu.make_async_copy(wqkv_hbm.at[:, pl.ds(c * QKV_CHUNK, QKV_CHUNK)], wq_buf.at[c], wq_sem.at[c])

    def wp_copy(c):
        return pltpu.make_async_copy(wproj_hbm.at[:, pl.ds(c * PROJ_CHUNK, PROJ_CHUNK)], wp_buf.at[c], wp_sem.at[c])

    def k_copy(i):
        rows = pl.ds(i * SEQ_CHUNK, SEQ_CHUNK)
        return pltpu.make_async_copy(k_hbm.at[rows], k_buf.at[rows], k_sem.at[i])

    def v_copy(i):
        rows = pl.ds(i * SEQ_CHUNK, SEQ_CHUNK)
        return pltpu.make_async_copy(v_hbm.at[rows], v_buf.at[rows], v_sem.at[i])

    def ko_copy(i):
        rows = pl.ds(i * SEQ_CHUNK, SEQ_CHUNK)
        return pltpu.make_async_copy(k_buf.at[rows], kout_hbm.at[rows], ko_sem.at[i])

    def vo_copy(i):
        rows = pl.ds(i * SEQ_CHUNK, SEQ_CHUNK)
        return pltpu.make_async_copy(v_buf.at[rows], vout_hbm.at[rows], vo_sem.at[i])

    for cp in small:
        cp.start()
    def fetch(n):
        if n < N_QKV:
            wq_copy(n).start()
        elif n < N_QKV + N_SEQ:
            k_copy(n - N_QKV).start()
            v_copy(n - N_QKV).start()
        elif n < N_QKV + N_SEQ + N_PROJ:
            wp_copy(n - N_QKV - N_SEQ).start()

    for n in range(WINDOW):
        fetch(n)

    for cp in small:
        cp.wait()
    x = x_ref[...].astype(F32)
    inv = lax.rsqrt(jnp.mean(x * x, axis=-1, keepdims=True) + EPS)
    act_buf[...] = (x * inv * ga_ref[...].astype(F32).reshape(1, HIDDEN)).astype(BF16)
    normed = act_buf[...]
    sub = lax.broadcasted_iota(jnp.int32, (8, HEAD_DIM), 0)
    tiles = []
    for t in range(ROWS // 8):
        tile = jnp.zeros((8, HEAD_DIM), jnp.int32)
        for r in range(8):
            tile = jnp.where(sub == r, len_ref[t * 8 + r], tile)
        tiles.append(tile)
    angles = jnp.concatenate(tiles, axis=0).astype(F32) * freq_ref[...]
    lane = lax.broadcasted_iota(jnp.int32, (ROWS, HEAD_DIM), 1)
    even = (lane % 2) == 0
    turned = lane < HEAD_DIM // 2
    cosine = jnp.where(turned, jnp.cos(angles), 1.0)
    sine = jnp.sin(angles)
    sine = jnp.where(turned, jnp.where(even, -sine, sine), 0.0)
    bias = b_ref[...].astype(F32).reshape(1, HIDDEN + 2 * KV * HEAD_DIM)

    def rotate(v):
        swapped = jnp.where(even, pltpu.roll(v, HEAD_DIM - 1, 1), pltpu.roll(v, 1, 1))
        return v * cosine + swapped * sine

    for c in range(N_QKV):
        wq_copy(c).wait()
        fetch(c + WINDOW)
        acc = jnp.dot(normed, wq_buf[c], preferred_element_type=F32) + bias[:, c * QKV_CHUNK:(c + 1) * QKV_CHUNK]
        for t in range(QKV_CHUNK // HEAD_DIM):
            head = c * (QKV_CHUNK // HEAD_DIM) + t
            part = acc[:, t * HEAD_DIM:(t + 1) * HEAD_DIM]
            if head < HEADS:
                q_scr[pl.ds(head, ROWS, stride=HEADS), :] = rotate(part)
            elif head < HEADS + KV:
                kn_scr[head - HEADS] = rotate(part)
            else:
                vn_scr[head - HEADS - KV] = part

    row16 = lax.broadcasted_iota(jnp.int32, (16, HEAD_DIM), 0)
    col = lax.broadcasted_iota(jnp.int32, (HEADS, FLAT), 1)
    row32 = lax.broadcasted_iota(jnp.int32, (2 * HEADS, HEAD_DIM), 0)
    head_row = lax.broadcasted_iota(jnp.int32, (HEADS, FLAT), 0)
    pos = jnp.where((col % KV) == (head_row // (HEADS // KV)), col // KV, 2 * LMAX)

    def chunk_body(i, carry):
        k_copy(i).wait()
        v_copy(i).wait()

        @pl.when(i + WINDOW < N_SEQ)
        def _():
            k_copy(i + WINDOW).start()
            v_copy(i + WINDOW).start()

        @pl.when(jnp.logical_and(i + WINDOW >= N_SEQ, i + WINDOW < N_SEQ + N_PROJ))
        def _():
            wp_copy(i + WINDOW - N_SEQ).start()

        for u in range(SEQ_CHUNK):
            b = i * SEQ_CHUNK + u
            ln = len_ref[b]
            base = pl.multiple_of((ln // 8) * 16, 16)
            hit = (row16 // 2) == (ln % 8)
            for buf, new in ((k_buf, kn_scr), (v_buf, vn_scr)):
                fresh = jnp.where(row16 % 2 == 0, new[0, pl.ds(b, 1), :], new[1, pl.ds(b, 1), :])
                old = buf[b, pl.ds(base, 16), :].astype(F32)
                buf[b, pl.ds(base, 16), :] = jnp.where(hit, fresh, old).astype(BF16)
        for s0 in range(0, SEQ_CHUNK, SUB):
            probs = []
            for u in range(s0, s0 + SUB, 2):
                b = i * SEQ_CHUNK + u
                q = q_scr[pl.ds(pl.multiple_of(b * HEADS, 2 * HEADS), 2 * HEADS), :]
                first = row32 < HEADS
                q2 = jnp.concatenate([jnp.where(first, q, 0.0), jnp.where(first, 0.0, q)], axis=1).astype(BF16)
                k2 = jnp.concatenate([k_buf[b], k_buf[b + 1]], axis=1)
                s2 = lax.dot_general(q2, k2, (((1,), (1,)), ((), ())), preferred_element_type=F32)
                pair = []
                for t in range(2):
                    s = jnp.where(pos <= len_ref[b + t], s2[t * HEADS:(t + 1) * HEADS], -jnp.inf)
                    e = jnp.exp((s - jnp.max(s, axis=1, keepdims=True)) * (HEAD_DIM ** -0.5))
                    pair.append((e * (1.0 / jnp.sum(e, axis=1, keepdims=True))).astype(BF16))
                probs.append(jnp.concatenate(pair, axis=0))
            for u in range(s0, s0 + SUB, 2):
                b = i * SEQ_CHUNK + u
                v2 = jnp.concatenate([v_buf[b], v_buf[b + 1]], axis=1)
                c2 = jnp.dot(probs[(u - s0) // 2], v2, preferred_element_type=F32)
                at = pl.multiple_of(b * HEADS, 2 * HEADS)
                ctx_scr[pl.ds(at, HEADS), :] = c2[:HEADS, :HEAD_DIM]
                ctx_scr[pl.ds(at + HEADS, HEADS), :] = c2[HEADS:, HEAD_DIM:]
        ko_copy(i).start()
        vo_copy(i).start()
        return carry

    lax.fori_loop(0, N_SEQ, chunk_body, 0)

    for h in range(HEADS):
        act_buf[:, h * HEAD_DIM:(h + 1) * HEAD_DIM] = ctx_scr[pl.ds(h, ROWS, stride=HEADS), :].astype(BF16)
    ctx = act_buf[...]
    total = jnp.zeros((ROWS, 1), F32)
    for c in range(N_PROJ):
        wp_copy(c).wait()
        cols = slice(c * PROJ_CHUNK, (c + 1) * PROJ_CHUNK)
        hid = x_ref[:, cols].astype(F32) + jnp.dot(ctx, wp_buf[c], preferred_element_type=F32)
        h_ref[:, cols] = hid
        total = total + jnp.sum(hid * hid, axis=-1, keepdims=True)
    inv2 = lax.rsqrt(total * (1.0 / HIDDEN) + EPS)
    m_ref[...] = (h_ref[...] * inv2 * gm_ref[...].astype(F32).reshape(1, HIDDEN)).astype(BF16)
    h_copy = pltpu.make_async_copy(h_ref, h_hbm, out_sem.at[0])
    m_copy = pltpu.make_async_copy(m_ref, m_hbm, out_sem.at[1])
    h_copy.start()
    m_copy.start()
    for i in range(N_SEQ):
        ko_copy(i).wait()
        vo_copy(i).wait()
    h_copy.wait()
    m_copy.wait()


def attention(lens, freq, x, ga, gm, bias, w_qkv, k_flat, v_flat, w_proj):
    hbm = pl.BlockSpec(memory_space=pl.ANY)
    smem = pl.BlockSpec(memory_space=pltpu.SMEM)
    dma = pltpu.SemaphoreType.DMA
    return pl.pallas_call(
        attn_kernel,
        out_shape=(jax.ShapeDtypeStruct((ROWS, HIDDEN), F32), jax.ShapeDtypeStruct((ROWS, HIDDEN), BF16),
                   jax.ShapeDtypeStruct(k_flat.shape, BF16), jax.ShapeDtypeStruct(v_flat.shape, BF16)),
        in_specs=[smem] + [hbm] * 9,
        out_specs=(hbm,) * 4,
        scratch_shapes=[
            pltpu.VMEM((1, HEAD_DIM), F32), pltpu.VMEM((ROWS, HIDDEN), BF16), pltpu.VMEM((HIDDEN,), BF16),
            pltpu.VMEM((HIDDEN,), BF16), pltpu.VMEM((HIDDEN + 2 * KV * HEAD_DIM,), BF16),
            pltpu.VMEM((ROWS, HIDDEN), F32), pltpu.VMEM((ROWS, HIDDEN), BF16),
            pltpu.VMEM((N_QKV, HIDDEN, QKV_CHUNK), BF16),
            pltpu.VMEM((N_PROJ, HIDDEN, PROJ_CHUNK), BF16),
            pltpu.VMEM((ROWS, FLAT, HEAD_DIM), BF16),
            pltpu.VMEM((ROWS, FLAT, HEAD_DIM), BF16),
            pltpu.VMEM((ROWS * HEADS, HEAD_DIM), F32),
            pltpu.VMEM((KV, ROWS, HEAD_DIM), F32),
            pltpu.VMEM((KV, ROWS, HEAD_DIM), F32),
            pltpu.VMEM((ROWS * HEADS, HEAD_DIM), F32),
            pltpu.VMEM((ROWS, HIDDEN), BF16),
            dma((5,)), dma((N_QKV,)), dma((N_PROJ,)), dma((N_SEQ,)), dma((N_SEQ,)), dma((N_SEQ,)), dma((N_SEQ,)), dma((2,)),
        ],
        compiler_params=pltpu.CompilerParams(vmem_limit_bytes=60 * 1024 * 1024),
        name="attn_block",
    )(lens, freq, x, ga, gm, bias, w_qkv, k_flat, v_flat, w_proj)


def mlp_kernel(m_hbm, h_hbm, win_hbm, wout_hbm, y_ref,
               m_ref, h_ref, rows_buf, win_buf, wout_buf, g_buf, pair_send, pair_recv, near_send, near_recv, far_keep, far_send, far_recv,
               own_acc, in_sem, win_sem, wout_sem, agx_s, agx_r, agp_s, agp_r, agr_s, agr_r,
               ps_s, ps_r, ns_s, ns_r, fs_s, fs_r):
    me = lax.axis_index('grp')
    partner = me + 1 - 2 * (me % 2)
    cross = (me + 2) % 4

    def win_copy(i, part, width):
        rows = pl.ds(i * F_CHUNK, width)
        return pltpu.make_async_copy(win_hbm.at[part, rows], win_buf.at[part, rows], win_sem.at[part, i])

    def wout_copy(j):
        cols = pl.ds(j * D_CHUNK, D_CHUNK)
        return pltpu.make_async_copy(wout_hbm.at[:, cols], wout_buf.at[:, cols], wout_sem.at[j])

    m_copy = pltpu.make_async_copy(m_hbm, m_ref, in_sem.at[0])
    h_copy = pltpu.make_async_copy(h_hbm, h_ref, in_sem.at[1])
    m_copy.start()
    tail = FFN_LOC - (N_F - 1) * F_CHUNK
    widths = [F_CHUNK] * (N_F - 1) + [tail]
    for i in range(N_F):
        for part in range(2):
            win_copy(i, part, widths[i]).start(priority=1)
    h_copy.start()

    barrier = pltpu.get_barrier_semaphore()
    for peer in (partner, cross):
        pl.semaphore_signal(barrier, inc=1, device_id={'grp': peer}, device_id_type=pl.DeviceIdType.MESH)
    pl.semaphore_wait(barrier, 2)

    def send(src, dst, ssem, rsem, peer):
        return pltpu.make_async_remote_copy(src_ref=src, dst_ref=dst, send_sem=ssem, recv_sem=rsem,
                                            device_id={'grp': peer}, device_id_type=pl.DeviceIdType.MESH)

    cross_copies = [send(m_ref.at[pl.ds(p * AG_ROWS, AG_ROWS)], rows_buf.at[pl.ds(2 * ROWS + p * AG_ROWS, AG_ROWS)],
                         agx_s.at[p], agx_r.at[p], cross) for p in range(AG_PIECES)]
    m_copy.wait()
    for cp in cross_copies:
        cp.start()
    pair_copy = send(m_ref, rows_buf.at[pl.ds(ROWS, ROWS)], agp_s, agp_r, partner)
    pair_copy.start()
    rows_buf[pl.ds(0, ROWS), :] = m_ref[...]
    relays = []
    for p in range(AG_PIECES):
        cross_copies[p].wait_recv()
        relay = send(rows_buf.at[pl.ds(2 * ROWS + p * AG_ROWS, AG_ROWS)],
                     rows_buf.at[pl.ds(3 * ROWS + p * AG_ROWS, AG_ROWS)], agr_s.at[p], agr_r.at[p], partner)
        relay.start()
        relays.append(relay)
    pair_copy.wait()
    for p in range(AG_PIECES):
        cross_copies[p].wait_send()
        relays[p].wait()

    def ffn_chunk(i, width):
        fr = pl.ds(i * F_CHUNK, width)
        rows = rows_buf[...]
        dims = (((1,), (1,)), ((), ()))
        gate = lax.dot_general(rows, win_buf[0, fr, :], dims, preferred_element_type=F32)
        up = lax.dot_general(rows, win_buf[1, fr, :], dims, preferred_element_type=F32)
        g_buf[:, fr] = (gate * jax.nn.sigmoid(gate) * up).astype(BF16)

    for j in range(N_D):
        wout_copy(j).start(priority=1)
    for i in range(N_F):
        for part in range(2):
            win_copy(i, part, widths[i]).wait()
    for i in range(N_F):
        ffn_chunk(i, widths[i])
    for j in range(N_D):
        wout_copy(j).wait()
    h_copy.wait()

    pair_copies = [send(pair_send.at[j], pair_recv.at[j], ps_s.at[j], ps_r.at[j], partner) for j in range(N_D)]
    near_copies = [send(near_send.at[j], near_recv.at[j], ns_s.at[j], ns_r.at[j], partner) for j in range(N_D)]
    far_copies = [send(far_send.at[j], far_recv.at[j], fs_s.at[j], fs_r.at[j], cross) for j in range(N_D)]

    def remote_block(j):
        cols = slice(j * D_CHUNK, (j + 1) * D_CHUNK)
        part = jnp.dot(g_buf[2 * ROWS:, :], wout_buf[:, cols], preferred_element_type=F32)
        far_keep[j] = part[:ROWS]
        pair_send[j] = part[ROWS:].astype(BF16)

    def local_block(j):
        cols = slice(j * D_CHUNK, (j + 1) * D_CHUNK)
        part = jnp.dot(g_buf[:2 * ROWS, :], wout_buf[:, cols], preferred_element_type=F32)
        own_acc[j] = part[:ROWS] + h_ref[:, cols]
        near_send[j] = part[ROWS:].astype(BF16)

    def pair_sum(j):
        pair_copies[j].wait_recv()
        far_send[j] = (far_keep[j] + pair_recv[j].astype(F32)).astype(BF16)

    half = N_D // 2
    for j in range(half):
        remote_block(j)
    for j in range(half):
        pair_copies[j].start()
    for j in range(half, N_D):
        remote_block(j)
    for j in range(half, N_D):
        pair_copies[j].start()
    for j in range(half):
        pair_sum(j)
    local_block(0)
    local_block(1)
    for j in range(half):
        far_copies[j].start()
    for j in range(2, half):
        local_block(j)
    for j in range(half, N_D):
        pair_sum(j)
    for j in range(half, N_D):
        local_block(j)
        far_copies[j].start()
    for j in range(N_D):
        near_copies[j].start()

    for j in range(N_D):
        cols = slice(j * D_CHUNK, (j + 1) * D_CHUNK)
        near_copies[j].wait_recv()
        far_copies[j].wait_recv()
        y_ref[:, cols] = (own_acc[j] + near_recv[j].astype(F32) + far_recv[j].astype(F32)).astype(BF16)
    for j in range(N_D):
        pair_copies[j].wait_send()
        near_copies[j].wait_send()
        far_copies[j].wait_send()


def mlp(m, h, w_in, w_out):
    vmem = pl.BlockSpec(memory_space=pltpu.VMEM)
    hbm = pl.BlockSpec(memory_space=pl.ANY)
    dma = pltpu.SemaphoreType.DMA
    piece = (N_D, ROWS, D_CHUNK)
    return pl.pallas_call(
        mlp_kernel,
        out_shape=jax.ShapeDtypeStruct((ROWS, HIDDEN), BF16),
        in_specs=[hbm] * 4,
        out_specs=vmem,
        scratch_shapes=[
            pltpu.VMEM((ROWS, HIDDEN), BF16), pltpu.VMEM((ROWS, HIDDEN), F32),
            pltpu.VMEM((4 * ROWS, HIDDEN), BF16),
            pltpu.VMEM((2, FFN_LOC, HIDDEN), BF16),
            pltpu.VMEM((FFN_LOC, HIDDEN), BF16),
            pltpu.VMEM((4 * ROWS, FFN_LOC), BF16),
            pltpu.VMEM(piece, BF16), pltpu.VMEM(piece, BF16),
            pltpu.VMEM(piece, BF16), pltpu.VMEM(piece, BF16),
            pltpu.VMEM(piece, F32), pltpu.VMEM(piece, BF16), pltpu.VMEM(piece, BF16),
            pltpu.VMEM(piece, F32),
            dma((2,)), dma((2, N_F)), dma((N_D,)),
            dma((AG_PIECES,)), dma((AG_PIECES,)), dma, dma, dma((AG_PIECES,)), dma((AG_PIECES,)),
            dma((N_D,)), dma((N_D,)), dma((N_D,)), dma((N_D,)), dma((N_D,)), dma((N_D,)),
        ],
        compiler_params=pltpu.CompilerParams(vmem_limit_bytes=60 * 1024 * 1024, collective_id=0, has_side_effects=True),
        name="mlp_block",
    )(m, h, w_in, w_out)


def rope_freq():
    pair = 2 * (np.arange(HEAD_DIM) // 2)
    return jnp.asarray((ROPE_BASE ** (-pair / (HEAD_DIM // 2)))[None, :], F32)


def solution(mesh):
    row_spec = P(('rep', 'grp'))
    repl_spec = P()

    def local_layer(x_in, seq_len, k_cache, v_cache, gamma_attn, w_qkv, b_qkv, w_proj, gamma_mlp, w_in, w_out):
        k_flat = k_cache.reshape(ROWS, FLAT, HEAD_DIM)
        v_flat = v_cache.reshape(ROWS, FLAT, HEAD_DIM)
        h, m, k_out, v_out = attention(seq_len, rope_freq(), x_in, gamma_attn, gamma_mlp, b_qkv, w_qkv, k_flat, v_flat, w_proj)
        layer_out = mlp(m, h, w_in, w_out)
        return layer_out, k_out.reshape(k_cache.shape), v_out.reshape(v_cache.shape)

    return jax.shard_map(local_layer, mesh=mesh,
                         in_specs=(row_spec, row_spec, row_spec, row_spec, repl_spec, repl_spec, repl_spec,
                                   repl_spec, repl_spec, P(None, 'grp', None), P('grp', None)),
                         out_specs=(row_spec, row_spec, row_spec), check_vma=False)
```

```python
import jax
import jax.numpy as jnp
import numpy as np
from jax import lax
from jax.experimental import pallas as pl
from jax.experimental.pallas import tpu as pltpu
from jax.sharding import PartitionSpec as P

HEAD_DIM = 128
ROPE_BASE = 10000.0
EPS = 1e-5
HIDDEN = 2048
HEADS = 16
KV = 2
ROWS = 64
LMAX = 256
FLAT = LMAX * KV
FFN_LOC = 2752
QKV_CHUNK = 512
N_QKV = 5
PROJ_CHUNK = 512
N_PROJ = 4
SEQ_CHUNK = 8
N_SEQ = ROWS // SEQ_CHUNK
WINDOW = 7
OUT_LAG = 3
F_CHUNK = 256
N_F = 11
D_EDGES = (0, 512, 1024, 1536, 2048)
N_D = len(D_EDGES) - 1
PAIR_LAG = 2
AG_PIECES = 4
AG_ROWS = ROWS // AG_PIECES
RING = 5
N_W = 4
W_ROWS = FFN_LOC // N_W
RELAY_AT = (6, 8, 10)
F32 = jnp.float32
BF16 = jnp.bfloat16


def attn_kernel(len_ref, freq_hbm, x_hbm, ga_hbm, gm_hbm, b_hbm, wqkv_hbm, k_hbm, v_hbm, wproj_hbm,
                h_hbm, m_hbm, kout_hbm, vout_hbm,
                freq_ref, x_ref, ga_ref, gm_ref, b_ref, h_ref, m_ref,
                wq_buf, wp_buf, k_buf, v_buf, q_scr, kn_scr, vn_scr, ctx_scr, act_buf,
                small_sem, wq_sem, wp_sem, k_sem, v_sem, out_sem):
    small = [pltpu.make_async_copy(src, dst, small_sem.at[n]) for n, (src, dst) in enumerate(
        ((x_hbm, x_ref), (ga_hbm, ga_ref), (freq_hbm, freq_ref), (b_hbm, b_ref), (gm_hbm, gm_ref)))]

    def wq_copy(c):
        return pltpu.make_async_copy(wqkv_hbm.at[:, pl.ds(c * QKV_CHUNK, QKV_CHUNK)], wq_buf.at[c], wq_sem.at[c])

    def wp_copy(c):
        return pltpu.make_async_copy(wproj_hbm.at[:, pl.ds(c * PROJ_CHUNK, PROJ_CHUNK)], wp_buf.at[c], wp_sem.at[c])

    def k_copy(i):
        rows = pl.ds(i * SEQ_CHUNK, SEQ_CHUNK)
        return pltpu.make_async_copy(k_hbm.at[rows], k_buf.at[rows], k_sem.at[i])

    def v_copy(i):
        rows = pl.ds(i * SEQ_CHUNK, SEQ_CHUNK)
        return pltpu.make_async_copy(v_hbm.at[rows], v_buf.at[rows], v_sem.at[i])

    def ko_copy(i):
        rows = pl.ds(i * SEQ_CHUNK, SEQ_CHUNK)
        return pltpu.make_async_copy(k_buf.at[rows], kout_hbm.at[rows], k_sem.at[i])

    def vo_copy(i):
        rows = pl.ds(i * SEQ_CHUNK, SEQ_CHUNK)
        return pltpu.make_async_copy(v_buf.at[rows], vout_hbm.at[rows], v_sem.at[i])

    for cp in small:
        cp.start()
    def fetch(n):
        if n < N_QKV:
            wq_copy(n).start()
        elif n < N_QKV + N_SEQ:
            k_copy(n - N_QKV).start()
            v_copy(n - N_QKV).start()
        elif n < N_QKV + N_SEQ + N_PROJ:
            wp_copy(n - N_QKV - N_SEQ).start()

    for n in range(WINDOW):
        fetch(n)

    for cp in small:
        cp.wait()
    x = x_ref[...].astype(F32)
    inv = lax.rsqrt(jnp.mean(x * x, axis=-1, keepdims=True) + EPS)
    act_buf[...] = (x * inv * ga_ref[...].astype(F32).reshape(1, HIDDEN)).astype(BF16)
    normed = act_buf[...]
    sub = lax.broadcasted_iota(jnp.int32, (8, HEAD_DIM), 0)
    tiles = []
    for t in range(ROWS // 8):
        tile = jnp.zeros((8, HEAD_DIM), jnp.int32)
        for r in range(8):
            tile = jnp.where(sub == r, len_ref[t * 8 + r], tile)
        tiles.append(tile)
    angles = jnp.concatenate(tiles, axis=0).astype(F32) * freq_ref[...]
    lane = lax.broadcasted_iota(jnp.int32, (ROWS, HEAD_DIM), 1)
    even = (lane % 2) == 0
    turned = lane < HEAD_DIM // 2
    cosine = jnp.where(turned, jnp.cos(angles), 1.0)
    sine = jnp.sin(angles)
    sine = jnp.where(turned, jnp.where(even, -sine, sine), 0.0)
    bias = b_ref[...].astype(F32).reshape(1, HIDDEN + 2 * KV * HEAD_DIM)

    def rotate(v):
        swapped = jnp.where(even, pltpu.roll(v, HEAD_DIM - 1, 1), pltpu.roll(v, 1, 1))
        return v * cosine + swapped * sine

    for c in range(N_QKV):
        wq_copy(c).wait()
        fetch(c + WINDOW)
        acc = jnp.dot(normed, wq_buf[c], preferred_element_type=F32) + bias[:, c * QKV_CHUNK:(c + 1) * QKV_CHUNK]
        for t in range(QKV_CHUNK // HEAD_DIM):
            head = c * (QKV_CHUNK // HEAD_DIM) + t
            part = acc[:, t * HEAD_DIM:(t + 1) * HEAD_DIM]
            if head < HEADS:
                q_scr[pl.ds(head, ROWS, stride=HEADS), :] = rotate(part)
            elif head < HEADS + KV:
                kn_scr[head - HEADS] = rotate(part)
            else:
                vn_scr[head - HEADS - KV] = part

    row16 = lax.broadcasted_iota(jnp.int32, (16, HEAD_DIM), 0)
    col = lax.broadcasted_iota(jnp.int32, (HEADS, FLAT), 1)
    row32 = lax.broadcasted_iota(jnp.int32, (2 * HEADS, HEAD_DIM), 0)
    head_row = lax.broadcasted_iota(jnp.int32, (HEADS, FLAT), 0)
    pos = jnp.where((col % KV) == (head_row // (HEADS // KV)), col // KV, 2 * LMAX)

    def insert(i):
        for u in range(SEQ_CHUNK):
            b = i * SEQ_CHUNK + u
            ln = len_ref[b]
            base = pl.multiple_of((ln // 8) * 16, 16)
            hit = (row16 // 2) == (ln % 8)
            for buf, new in ((k_buf, kn_scr), (v_buf, vn_scr)):
                fresh = jnp.where(row16 % 2 == 0, new[0, pl.ds(b, 1), :], new[1, pl.ds(b, 1), :])
                old = buf[b, pl.ds(base, 16), :].astype(F32)
                buf[b, pl.ds(base, 16), :] = jnp.where(hit, fresh, old).astype(BF16)

    def scores(i):
        out = []
        for u in range(0, SEQ_CHUNK, 2):
            b = i * SEQ_CHUNK + u
            q = q_scr[pl.ds(b * HEADS, 2 * HEADS), :]
            first = row32 < HEADS
            q2 = jnp.concatenate([jnp.where(first, q, 0.0), jnp.where(first, 0.0, q)], axis=1).astype(BF16)
            k2 = jnp.concatenate([k_buf[b], k_buf[b + 1]], axis=1)
            out.append(lax.dot_general(q2, k2, (((1,), (1,)), ((), ())), preferred_element_type=F32))
        return out

    def probabilities(i, raw):
        probs = []
        for u in range(0, SEQ_CHUNK, 2):
            b = i * SEQ_CHUNK + u
            s2 = raw[u // 2]
            pair = []
            for t in range(2):
                s = jnp.where(pos <= len_ref[b + t], s2[t * HEADS:(t + 1) * HEADS], -jnp.inf)
                e = jnp.exp((s - jnp.max(s, axis=1, keepdims=True)) * (HEAD_DIM ** -0.5))
                pair.append((e * (1.0 / jnp.sum(e, axis=1, keepdims=True))).astype(BF16))
            probs.append(jnp.concatenate(pair, axis=0))
        return probs

    def weighted_values(i, probs):
        for u in range(0, SEQ_CHUNK, 2):
            b = i * SEQ_CHUNK + u
            v2 = jnp.concatenate([v_buf[b], v_buf[b + 1]], axis=1)
            c2 = jnp.dot(probs[u // 2], v2, preferred_element_type=F32)
            ctx_scr[pl.ds(b * HEADS, HEADS), :] = c2[:HEADS, :HEAD_DIM]
            ctx_scr[pl.ds((b + 1) * HEADS, HEADS), :] = c2[HEADS:, HEAD_DIM:]

    probs = None
    for i in range(N_SEQ):
        k_copy(i).wait()
        v_copy(i).wait()
        fetch(N_QKV + i + WINDOW)
        if i >= OUT_LAG:
            ko_copy(i - OUT_LAG).start()
            vo_copy(i - OUT_LAG).start()
        insert(i)
        raw = scores(i)
        if i > 0:
            weighted_values(i - 1, probs)
        probs = probabilities(i, raw)
    for i in range(N_SEQ - OUT_LAG, N_SEQ):
        ko_copy(i).start()
        vo_copy(i).start()
    weighted_values(N_SEQ - 1, probs)

    for h in range(HEADS):
        act_buf[:, h * HEAD_DIM:(h + 1) * HEAD_DIM] = ctx_scr[pl.ds(h, ROWS, stride=HEADS), :].astype(BF16)
    ctx = act_buf[...]
    total = jnp.zeros((ROWS, 1), F32)
    for c in range(N_PROJ):
        wp_copy(c).wait()
        cols = slice(c * PROJ_CHUNK, (c + 1) * PROJ_CHUNK)
        hid = x_ref[:, cols].astype(F32) + jnp.dot(ctx, wp_buf[c], preferred_element_type=F32)
        h_ref[:, cols] = hid
        total = total + jnp.sum(hid * hid, axis=-1, keepdims=True)
    inv2 = lax.rsqrt(total * (1.0 / HIDDEN) + EPS)
    m_ref[...] = (h_ref[...] * inv2 * gm_ref[...].astype(F32).reshape(1, HIDDEN)).astype(BF16)
    h_copy = pltpu.make_async_copy(h_ref, h_hbm, out_sem.at[0])
    m_copy = pltpu.make_async_copy(m_ref, m_hbm, out_sem.at[1])
    h_copy.start()
    m_copy.start()
    for i in range(N_SEQ):
        ko_copy(i).wait()
        vo_copy(i).wait()
    h_copy.wait()
    m_copy.wait()


def attention(lens, freq, x, ga, gm, bias, w_qkv, k_flat, v_flat, w_proj):
    hbm = pl.BlockSpec(memory_space=pl.ANY)
    smem = pl.BlockSpec(memory_space=pltpu.SMEM)
    dma = pltpu.SemaphoreType.DMA
    return pl.pallas_call(
        attn_kernel,
        out_shape=(jax.ShapeDtypeStruct((ROWS, HIDDEN), F32), jax.ShapeDtypeStruct((ROWS, HIDDEN), BF16),
                   jax.ShapeDtypeStruct(k_flat.shape, BF16), jax.ShapeDtypeStruct(v_flat.shape, BF16)),
        in_specs=[smem] + [hbm] * 9,
        out_specs=(hbm,) * 4,
        scratch_shapes=[
            pltpu.VMEM((1, HEAD_DIM), F32), pltpu.VMEM((ROWS, HIDDEN), BF16), pltpu.VMEM((HIDDEN,), BF16),
            pltpu.VMEM((HIDDEN,), BF16), pltpu.VMEM((HIDDEN + 2 * KV * HEAD_DIM,), BF16),
            pltpu.VMEM((ROWS, HIDDEN), F32), pltpu.VMEM((ROWS, HIDDEN), BF16),
            pltpu.VMEM((N_QKV, HIDDEN, QKV_CHUNK), BF16),
            pltpu.VMEM((N_PROJ, HIDDEN, PROJ_CHUNK), BF16),
            pltpu.VMEM((ROWS, FLAT, HEAD_DIM), BF16),
            pltpu.VMEM((ROWS, FLAT, HEAD_DIM), BF16),
            pltpu.VMEM((ROWS * HEADS, HEAD_DIM), F32),
            pltpu.VMEM((KV, ROWS, HEAD_DIM), F32),
            pltpu.VMEM((KV, ROWS, HEAD_DIM), F32),
            pltpu.VMEM((ROWS * HEADS, HEAD_DIM), F32),
            pltpu.VMEM((ROWS, HIDDEN), BF16),
            dma((5,)), dma((N_QKV,)), dma((N_PROJ,)), dma((N_SEQ,)), dma((N_SEQ,)), dma((2,)),
        ],
        compiler_params=pltpu.CompilerParams(vmem_limit_bytes=60 * 1024 * 1024),
        name="attn_block",
    )(lens, freq, x, ga, gm, bias, w_qkv, k_flat, v_flat, w_proj)


def mlp_kernel(m_hbm, h_hbm, win_hbm, wout_hbm, y_ref,
               m_ref, h_ref, rows_buf, win_buf, wint_buf, wout_buf, g_buf, pair_send, pair_recv, near_send, near_recv, far_keep, far_send, far_recv,
               own_acc, in_sem, win_sem, wout_sem, agx_s, agx_r, agp_s, agp_r, agr_s, agr_r,
               ps_s, ps_r, ns_s, ns_r, fs_s, fs_r):
    me = lax.axis_index('grp')
    partner = me + 1 - 2 * (me % 2)
    cross = (me + 2) % 4

    def win_copy(i, width):
        src = win_hbm.at[:, pl.ds(i * F_CHUNK, width)]
        return pltpu.make_async_copy(src, win_buf.at[i % RING, :, pl.ds(0, width)], win_sem.at[i % RING])

    def wout_copy(j):
        rows = pl.ds(j * W_ROWS, W_ROWS)
        return pltpu.make_async_copy(wout_hbm.at[rows], wout_buf.at[rows], wout_sem.at[j])

    m_copy = pltpu.make_async_copy(m_hbm, m_ref, in_sem.at[0])
    h_copy = pltpu.make_async_copy(h_hbm, h_ref, in_sem.at[1])
    m_copy.start()
    tail = FFN_LOC - (N_F - 1) * F_CHUNK
    widths = [F_CHUNK] * (N_F - 1) + [tail]
    for i in range(RING):
        win_copy(i, widths[i]).start(priority=1)
    h_copy.start()

    barrier = pltpu.get_barrier_semaphore()
    for peer in (partner, cross):
        pl.semaphore_signal(barrier, inc=1, device_id={'grp': peer}, device_id_type=pl.DeviceIdType.MESH)
    pl.semaphore_wait(barrier, 2)

    def send(src, dst, ssem, rsem, peer):
        return pltpu.make_async_remote_copy(src_ref=src, dst_ref=dst, send_sem=ssem, recv_sem=rsem,
                                            device_id={'grp': peer}, device_id_type=pl.DeviceIdType.MESH)

    cross_copies = [send(m_ref.at[pl.ds(p * AG_ROWS, AG_ROWS)], rows_buf.at[pl.ds(2 * ROWS + p * AG_ROWS, AG_ROWS)],
                         agx_s.at[p], agx_r.at[p], cross) for p in range(AG_PIECES)]
    m_copy.wait()
    for cp in cross_copies:
        cp.start()
    pair_copy = send(m_ref, rows_buf.at[pl.ds(ROWS, ROWS)], agp_s, agp_r, partner)
    pair_copy.start()
    rows_buf[pl.ds(0, ROWS), :] = m_ref[...]
    relays = [send(rows_buf.at[pl.ds(2 * ROWS + p * AG_ROWS, AG_ROWS)],
                   rows_buf.at[pl.ds(3 * ROWS + p * AG_ROWS, AG_ROWS)], agr_s.at[p], agr_r.at[p], partner)
              for p in range(AG_PIECES)]

    def swiglu(rows, i, width, top, weights):
        gate = jnp.dot(rows, weights[0], preferred_element_type=F32)
        up = jnp.dot(rows, weights[1], preferred_element_type=F32)
        g_buf[pl.ds(top, 2 * ROWS), pl.ds(i * F_CHUNK, width)] = (gate * jax.nn.sigmoid(gate) * up).astype(BF16)

    for i in range(N_F):
        win_copy(i, widths[i]).wait()
        for part in range(2):
            wint_buf[i, part, :, :widths[i]] = win_buf[i % RING, part, :widths[i], :].T
        if i + RING < N_F:
            win_copy(i + RING, widths[i + RING]).start(priority=1)
        if i == 1:
            pair_copy.wait()
        if i >= 1:
            swiglu(rows_buf[pl.ds(0, 2 * ROWS), :], i - 1, F_CHUNK, 0, [wint_buf[i - 1, part] for part in range(2)])
        if i in RELAY_AT:
            p = RELAY_AT.index(i)
            cross_copies[p].wait_recv()
            relays[p].start()
    swiglu(rows_buf[pl.ds(0, 2 * ROWS), :], N_F - 1, tail, 0, [wint_buf[N_F - 1, part, :, :tail] for part in range(2)])
    for j in range(N_W):
        wout_copy(j).start(priority=1)
    for p in range(len(RELAY_AT), AG_PIECES):
        cross_copies[p].wait_recv()
        relays[p].start()
    for p in range(AG_PIECES):
        cross_copies[p].wait_send()
        relays[p].wait()
    for i in range(N_F):
        swiglu(rows_buf[pl.ds(2 * ROWS, 2 * ROWS), :], i, widths[i], 2 * ROWS,
               [wint_buf[i, part, :, :widths[i]] for part in range(2)])
    for j in range(N_W):
        wout_copy(j).wait()
    h_copy.wait()

    def piece(k):
        return pl.ds(D_EDGES[k], D_EDGES[k + 1] - D_EDGES[k])

    def block_send(src, dst, ssem, rsem, peer):
        return [send(src.at[:, piece(k)], dst.at[:, piece(k)], ssem.at[k], rsem.at[k], peer) for k in range(N_D)]

    pair_copies = block_send(pair_send, pair_recv, ps_s, ps_r, partner)
    near_copies = block_send(near_send, near_recv, ns_s, ns_r, partner)
    far_copies = block_send(far_send, far_recv, fs_s, fs_r, cross)

    def remote_block(k):
        part = jnp.dot(g_buf[2 * ROWS:, :], wout_buf[:, piece(k)], preferred_element_type=F32)
        far_keep[:, piece(k)] = part[:ROWS]
        pair_send[:, piece(k)] = part[ROWS:].astype(BF16)
        pair_copies[k].start()

    def local_block(k):
        part = jnp.dot(g_buf[:2 * ROWS, :], wout_buf[:, piece(k)], preferred_element_type=F32)
        own_acc[:, piece(k)] = part[:ROWS] + h_ref[:, piece(k)]
        near_send[:, piece(k)] = part[ROWS:].astype(BF16)
        near_copies[k].start()

    def pair_sum(k):
        pair_copies[k].wait_recv()
        far_send[:, piece(k)] = (far_keep[:, piece(k)] + pair_recv[:, piece(k)].astype(F32)).astype(BF16)
        far_copies[k].start()

    steps = [(remote_block, k) for k in range(N_D)] + [(local_block, k) for k in range(N_D)]
    for n, (step, k) in enumerate(steps):
        step(k)
        if 0 <= n - PAIR_LAG < N_D:
            pair_sum(n - PAIR_LAG)
    for k in range(N_D):
        near_copies[k].wait_recv()
        far_copies[k].wait_recv()
        y_ref[:, piece(k)] = (own_acc[:, piece(k)] + near_recv[:, piece(k)].astype(F32)
                              + far_recv[:, piece(k)].astype(F32)).astype(BF16)
    for k in range(N_D):
        pair_copies[k].wait_send()
        near_copies[k].wait_send()
        far_copies[k].wait_send()


def mlp(m, h, w_in, w_out):
    vmem = pl.BlockSpec(memory_space=pltpu.VMEM)
    hbm = pl.BlockSpec(memory_space=pl.ANY)
    dma = pltpu.SemaphoreType.DMA
    piece = (ROWS, HIDDEN)
    return pl.pallas_call(
        mlp_kernel,
        out_shape=jax.ShapeDtypeStruct((ROWS, HIDDEN), BF16),
        in_specs=[hbm] * 4,
        out_specs=vmem,
        scratch_shapes=[
            pltpu.VMEM((ROWS, HIDDEN), BF16), pltpu.VMEM((ROWS, HIDDEN), F32),
            pltpu.VMEM((4 * ROWS, HIDDEN), BF16),
            pltpu.VMEM((RING, 2, F_CHUNK, HIDDEN), BF16),
            pltpu.VMEM((N_F, 2, HIDDEN, F_CHUNK), BF16),
            pltpu.VMEM((FFN_LOC, HIDDEN), BF16),
            pltpu.VMEM((4 * ROWS, FFN_LOC), BF16),
            pltpu.VMEM(piece, BF16), pltpu.VMEM(piece, BF16),
            pltpu.VMEM(piece, BF16), pltpu.VMEM(piece, BF16),
            pltpu.VMEM(piece, F32), pltpu.VMEM(piece, BF16), pltpu.VMEM(piece, BF16),
            pltpu.VMEM(piece, F32),
            dma((2,)), dma((RING,)), dma((N_W,)),
            dma((AG_PIECES,)), dma((AG_PIECES,)), dma, dma, dma((AG_PIECES,)), dma((AG_PIECES,)),
            dma((N_D,)), dma((N_D,)), dma((N_D,)), dma((N_D,)), dma((N_D,)), dma((N_D,)),
        ],
        compiler_params=pltpu.CompilerParams(vmem_limit_bytes=60 * 1024 * 1024, collective_id=0, has_side_effects=True),
        name="mlp_block",
    )(m, h, w_in, w_out)


def rope_freq():
    pair = 2 * (np.arange(HEAD_DIM) // 2)
    return jnp.asarray((ROPE_BASE ** (-pair / (HEAD_DIM // 2)))[None, :], F32)


def solution(mesh):
    row_spec = P(('rep', 'grp'))
    repl_spec = P()

    def local_layer(x_in, seq_len, k_cache, v_cache, gamma_attn, w_qkv, b_qkv, w_proj, gamma_mlp, w_in, w_out):
        k_flat = k_cache.reshape(ROWS, FLAT, HEAD_DIM)
        v_flat = v_cache.reshape(ROWS, FLAT, HEAD_DIM)
        h, m, k_out, v_out = attention(seq_len, rope_freq(), x_in, gamma_attn, gamma_mlp, b_qkv, w_qkv, k_flat, v_flat, w_proj)
        layer_out = mlp(m, h, w_in, w_out)
        return layer_out, k_out.reshape(k_cache.shape), v_out.reshape(v_cache.shape)

    return jax.shard_map(local_layer, mesh=mesh,
                         in_specs=(row_spec, row_spec, row_spec, row_spec, repl_spec, repl_spec, repl_spec,
                                   repl_spec, repl_spec, P(None, 'grp', None), P('grp', None)),
                         out_specs=(row_spec, row_spec, row_spec), check_vma=False)
```

```python
import jax
import jax.numpy as jnp
import numpy as np
from jax import lax
from jax.experimental import pallas as pl
from jax.experimental.pallas import tpu as pltpu
from jax.sharding import PartitionSpec as P

HEAD_DIM = 128
ROPE_BASE = 10000.0
EPS = 1e-5
HIDDEN = 2048
HEADS = 16
KV = 2
ROWS = 64
LMAX = 256
FLAT = LMAX * KV
FFN_LOC = 2752
QKV_CHUNK = 512
N_QKV = 5
PROJ_CHUNK = 512
N_PROJ = 4
SEQ_CHUNK = 8
N_SEQ = ROWS // SEQ_CHUNK
WINDOW = 7
OUT_LAG = 4
F_CHUNK = 256
N_F = 11
D_EDGES = (0, 512, 1024, 1536, 2048)
N_D = len(D_EDGES) - 1
PAIR_LAG = 2
AG_PIECES = 4
AG_COLS = HIDDEN // AG_PIECES
K_PARTS = ((0, HIDDEN // 2), (HIDDEN // 2, HIDDEN // 2))
RING = 4
CUT = 6
N_T = 9
N_W = 4
W_ROWS = FFN_LOC // N_W
RELAY_AT = (5, 7)
HBM_ROWS = 2048
F32 = jnp.float32
BF16 = jnp.bfloat16


def attn_kernel(len_ref, freq_hbm, x_hbm, ga_hbm, gm_hbm, b_hbm, wqkv_hbm, k_hbm, v_hbm, wproj_hbm,
                h_hbm, m_hbm, kout_hbm, vout_hbm,
                freq_ref, x_ref, ga_ref, gm_ref, b_ref, h_ref, m_ref,
                wq_buf, wp_buf, k_buf, v_buf, q_scr, kn_scr, vn_scr, ctx_scr, act_buf,
                small_sem, wq_sem, wp_sem, k_sem, v_sem, out_sem):
    small = [pltpu.make_async_copy(src, dst, small_sem.at[n]) for n, (src, dst) in enumerate(
        ((x_hbm, x_ref), (ga_hbm, ga_ref), (freq_hbm, freq_ref), (b_hbm, b_ref), (gm_hbm, gm_ref)))]

    def wq_copy(c):
        return pltpu.make_async_copy(wqkv_hbm.at[:, pl.ds(c * QKV_CHUNK, QKV_CHUNK)], wq_buf.at[c], wq_sem.at[c])

    def wp_copy(c):
        return pltpu.make_async_copy(wproj_hbm.at[:, pl.ds(c * PROJ_CHUNK, PROJ_CHUNK)], wp_buf.at[c], wp_sem.at[c])

    def k_copy(i):
        rows = pl.ds(i * SEQ_CHUNK, SEQ_CHUNK)
        return pltpu.make_async_copy(k_hbm.at[rows], k_buf.at[rows], k_sem.at[i])

    def v_copy(i):
        rows = pl.ds(i * SEQ_CHUNK, SEQ_CHUNK)
        return pltpu.make_async_copy(v_hbm.at[rows], v_buf.at[rows], v_sem.at[i])

    def ko_copy(i):
        rows = pl.ds(i * SEQ_CHUNK, SEQ_CHUNK)
        return pltpu.make_async_copy(k_buf.at[rows], kout_hbm.at[rows], k_sem.at[i])

    def vo_copy(i):
        rows = pl.ds(i * SEQ_CHUNK, SEQ_CHUNK)
        return pltpu.make_async_copy(v_buf.at[rows], vout_hbm.at[rows], v_sem.at[i])

    for cp in small:
        cp.start()
    def fetch(n):
        if n < N_QKV:
            wq_copy(n).start()
        elif n < N_QKV + N_SEQ:
            k_copy(n - N_QKV).start()
            v_copy(n - N_QKV).start()
        elif n < N_QKV + N_SEQ + N_PROJ:
            wp_copy(n - N_QKV - N_SEQ).start()

    for n in range(WINDOW):
        fetch(n)

    for cp in small:
        cp.wait()
    x = x_ref[...].astype(F32)
    inv = lax.rsqrt(jnp.mean(x * x, axis=-1, keepdims=True) + EPS)
    act_buf[...] = (x * inv * ga_ref[...].astype(F32).reshape(1, HIDDEN)).astype(BF16)
    normed = act_buf[...]
    sub = lax.broadcasted_iota(jnp.int32, (8, HEAD_DIM), 0)
    tiles = []
    for t in range(ROWS // 8):
        tile = jnp.zeros((8, HEAD_DIM), jnp.int32)
        for r in range(8):
            tile = jnp.where(sub == r, len_ref[t * 8 + r], tile)
        tiles.append(tile)
    angles = jnp.concatenate(tiles, axis=0).astype(F32) * freq_ref[...]
    lane = lax.broadcasted_iota(jnp.int32, (ROWS, HEAD_DIM), 1)
    even = (lane % 2) == 0
    turned = lane < HEAD_DIM // 2
    cosine = jnp.where(turned, jnp.cos(angles), 1.0)
    sine = jnp.sin(angles)
    sine = jnp.where(turned, jnp.where(even, -sine, sine), 0.0)
    bias = b_ref[...].astype(F32).reshape(1, HIDDEN + 2 * KV * HEAD_DIM)

    def rotate(v):
        swapped = jnp.where(even, pltpu.roll(v, HEAD_DIM - 1, 1), pltpu.roll(v, 1, 1))
        return v * cosine + swapped * sine

    for c in range(N_QKV):
        wq_copy(c).wait()
        fetch(c + WINDOW)
        acc = jnp.dot(normed, wq_buf[c], preferred_element_type=F32) + bias[:, c * QKV_CHUNK:(c + 1) * QKV_CHUNK]
        for t in range(QKV_CHUNK // HEAD_DIM):
            head = c * (QKV_CHUNK // HEAD_DIM) + t
            part = acc[:, t * HEAD_DIM:(t + 1) * HEAD_DIM]
            if head < HEADS:
                q_scr[pl.ds(head, ROWS, stride=HEADS), :] = rotate(part)
            elif head < HEADS + KV:
                kn_scr[head - HEADS] = rotate(part)
            else:
                vn_scr[head - HEADS - KV] = part

    row16 = lax.broadcasted_iota(jnp.int32, (16, HEAD_DIM), 0)
    col = lax.broadcasted_iota(jnp.int32, (HEADS, FLAT), 1)
    row32 = lax.broadcasted_iota(jnp.int32, (2 * HEADS, HEAD_DIM), 0)
    head_row = lax.broadcasted_iota(jnp.int32, (HEADS, FLAT), 0)
    pos = jnp.where((col % KV) == (head_row // (HEADS // KV)), col // KV, 2 * LMAX)

    def insert(i):
        for u in range(SEQ_CHUNK):
            b = i * SEQ_CHUNK + u
            ln = len_ref[b]
            base = pl.multiple_of((ln // 8) * 16, 16)
            hit = (row16 // 2) == (ln % 8)
            for buf, new in ((k_buf, kn_scr), (v_buf, vn_scr)):
                fresh = jnp.where(row16 % 2 == 0, new[0, pl.ds(b, 1), :], new[1, pl.ds(b, 1), :])
                old = buf[b, pl.ds(base, 16), :].astype(F32)
                buf[b, pl.ds(base, 16), :] = jnp.where(hit, fresh, old).astype(BF16)

    def scores(i):
        out = []
        for u in range(0, SEQ_CHUNK, 2):
            b = i * SEQ_CHUNK + u
            q = q_scr[pl.ds(b * HEADS, 2 * HEADS), :]
            first = row32 < HEADS
            q2 = jnp.concatenate([jnp.where(first, q, 0.0), jnp.where(first, 0.0, q)], axis=1).astype(BF16)
            k2 = jnp.concatenate([k_buf[b], k_buf[b + 1]], axis=1)
            out.append(lax.dot_general(q2, k2, (((1,), (1,)), ((), ())), preferred_element_type=F32))
        return out

    def probabilities(i, raw):
        probs = []
        for u in range(0, SEQ_CHUNK, 2):
            b = i * SEQ_CHUNK + u
            s2 = raw[u // 2]
            pair = []
            for t in range(2):
                s = jnp.where(pos <= len_ref[b + t], s2[t * HEADS:(t + 1) * HEADS], -jnp.inf)
                e = jnp.exp((s - jnp.max(s, axis=1, keepdims=True)) * (HEAD_DIM ** -0.5))
                pair.append((e * (1.0 / jnp.sum(e, axis=1, keepdims=True))).astype(BF16))
            probs.append(jnp.concatenate(pair, axis=0))
        return probs

    def weighted_values(i, probs):
        for u in range(0, SEQ_CHUNK, 2):
            b = i * SEQ_CHUNK + u
            v2 = jnp.concatenate([v_buf[b], v_buf[b + 1]], axis=1)
            c2 = jnp.dot(probs[u // 2], v2, preferred_element_type=F32)
            ctx_scr[pl.ds(b * HEADS, HEADS), :] = c2[:HEADS, :HEAD_DIM]
            ctx_scr[pl.ds((b + 1) * HEADS, HEADS), :] = c2[HEADS:, HEAD_DIM:]

    probs = None
    for i in range(N_SEQ):
        k_copy(i).wait()
        v_copy(i).wait()
        fetch(N_QKV + i + WINDOW)
        if i >= OUT_LAG:
            ko_copy(i - OUT_LAG).start()
            vo_copy(i - OUT_LAG).start()
        insert(i)
        raw = scores(i)
        if i > 0:
            weighted_values(i - 1, probs)
        probs = probabilities(i, raw)
    for i in range(N_SEQ - OUT_LAG, N_SEQ):
        ko_copy(i).start()
        vo_copy(i).start()
    weighted_values(N_SEQ - 1, probs)

    for h in range(HEADS):
        act_buf[:, h * HEAD_DIM:(h + 1) * HEAD_DIM] = ctx_scr[pl.ds(h, ROWS, stride=HEADS), :].astype(BF16)
    ctx = act_buf[...]
    total = jnp.zeros((ROWS, 1), F32)
    for c in range(N_PROJ):
        wp_copy(c).wait()
        cols = slice(c * PROJ_CHUNK, (c + 1) * PROJ_CHUNK)
        hid = x_ref[:, cols].astype(F32) + jnp.dot(ctx, wp_buf[c], preferred_element_type=F32)
        h_ref[:, cols] = hid
        total = total + jnp.sum(hid * hid, axis=-1, keepdims=True)
    inv2 = lax.rsqrt(total * (1.0 / HIDDEN) + EPS)
    m_ref[...] = (h_ref[...] * inv2 * gm_ref[...].astype(F32).reshape(1, HIDDEN)).astype(BF16)
    h_copy = pltpu.make_async_copy(h_ref, h_hbm.at[pl.ds(0, ROWS)], out_sem.at[0])
    m_copy = pltpu.make_async_copy(m_ref, m_hbm.at[pl.ds(0, ROWS)], out_sem.at[1])
    h_copy.start()
    m_copy.start()
    for i in range(N_SEQ):
        ko_copy(i).wait()
        vo_copy(i).wait()
    h_copy.wait()
    m_copy.wait()


def attention(lens, freq, x, ga, gm, bias, w_qkv, k_flat, v_flat, w_proj):
    hbm = pl.BlockSpec(memory_space=pl.ANY)
    smem = pl.BlockSpec(memory_space=pltpu.SMEM)
    dma = pltpu.SemaphoreType.DMA
    return pl.pallas_call(
        attn_kernel,
        out_shape=(jax.ShapeDtypeStruct((HBM_ROWS, HIDDEN), F32), jax.ShapeDtypeStruct((HBM_ROWS, HIDDEN), BF16),
                   jax.ShapeDtypeStruct(k_flat.shape, BF16), jax.ShapeDtypeStruct(v_flat.shape, BF16)),
        in_specs=[smem] + [hbm] * 9,
        out_specs=(hbm,) * 4,
        scratch_shapes=[
            pltpu.VMEM((1, HEAD_DIM), F32), pltpu.VMEM((ROWS, HIDDEN), BF16), pltpu.VMEM((HIDDEN,), BF16),
            pltpu.VMEM((HIDDEN,), BF16), pltpu.VMEM((HIDDEN + 2 * KV * HEAD_DIM,), BF16),
            pltpu.VMEM((ROWS, HIDDEN), F32), pltpu.VMEM((ROWS, HIDDEN), BF16),
            pltpu.VMEM((N_QKV, HIDDEN, QKV_CHUNK), BF16),
            pltpu.VMEM((N_PROJ, HIDDEN, PROJ_CHUNK), BF16),
            pltpu.VMEM((ROWS, FLAT, HEAD_DIM), BF16),
            pltpu.VMEM((ROWS, FLAT, HEAD_DIM), BF16),
            pltpu.VMEM((ROWS * HEADS, HEAD_DIM), F32),
            pltpu.VMEM((KV, ROWS, HEAD_DIM), F32),
            pltpu.VMEM((KV, ROWS, HEAD_DIM), F32),
            pltpu.VMEM((ROWS * HEADS, HEAD_DIM), F32),
            pltpu.VMEM((ROWS, HIDDEN), BF16),
            dma((5,)), dma((N_QKV,)), dma((N_PROJ,)), dma((N_SEQ,)), dma((N_SEQ,)), dma((2,)),
        ],
        compiler_params=pltpu.CompilerParams(vmem_limit_bytes=60 * 1024 * 1024),
        name="attn_block",
    )(lens, freq, x, ga, gm, bias, w_qkv, k_flat, v_flat, w_proj)


def mlp_kernel(m_hbm, h_hbm, win_hbm, wout_hbm, y_ref,
               m_ref, h_ref, rows_buf, part_acc, late_acc, win_buf, wint_buf, wout_buf, g_buf, pair_send, pair_recv, near_send, near_recv, far_keep, far_send, far_recv,
               own_acc, in_sem, win_sem, wout_sem, agx_s, agx_r, agp_s, agp_r, agr_s, agr_r,
               ps_s, ps_r, ns_s, ns_r, fs_s, fs_r):
    me = lax.axis_index('grp')
    partner = me + 1 - 2 * (me % 2)
    cross = (me + 2) % 4

    def win_copy(i, width):
        src = win_hbm.at[:, pl.ds(i * F_CHUNK, width)]
        return pltpu.make_async_copy(src, win_buf.at[i % RING, :, pl.ds(0, width)], win_sem.at[i % RING])

    def wout_copy(j):
        rows = pl.ds(j * W_ROWS, W_ROWS)
        return pltpu.make_async_copy(wout_hbm.at[rows], wout_buf.at[rows], wout_sem.at[j])

    m_copy = pltpu.make_async_copy(m_hbm.at[pl.ds(0, ROWS)], m_ref, in_sem.at[0])
    h_copy = pltpu.make_async_copy(h_hbm.at[pl.ds(0, ROWS)], h_ref, in_sem.at[1])
    m_copy.start()
    tail = FFN_LOC - (N_F - 1) * F_CHUNK
    widths = [F_CHUNK] * (N_F - 1) + [tail]
    for i in range(RING):
        win_copy(i, widths[i]).start(priority=1)
    h_copy.start()

    barrier = pltpu.get_barrier_semaphore()
    for peer in (partner, cross):
        pl.semaphore_signal(barrier, inc=1, device_id={'grp': peer}, device_id_type=pl.DeviceIdType.MESH)
    pl.semaphore_wait(barrier, 2)

    def send(src, dst, ssem, rsem, peer):
        return pltpu.make_async_remote_copy(src_ref=src, dst_ref=dst, send_sem=ssem, recv_sem=rsem,
                                            device_id={'grp': peer}, device_id_type=pl.DeviceIdType.MESH)

    def part_of(slot, p):
        return rows_buf.at[pl.ds(slot * ROWS, ROWS), pl.ds(p * AG_COLS, AG_COLS)]

    cross_copies = [send(m_ref.at[:, pl.ds(p * AG_COLS, AG_COLS)], part_of(2, p), agx_s.at[p], agx_r.at[p], cross)
                    for p in range(AG_PIECES)]
    m_copy.wait()
    for cp in cross_copies:
        cp.start()
    pair_copy = send(m_ref, rows_buf.at[pl.ds(ROWS, ROWS)], agp_s, agp_r, partner)
    pair_copy.start()
    rows_buf[pl.ds(0, ROWS), :] = m_ref[...]
    relays = [send(part_of(2, p), part_of(3, p), agr_s.at[p], agr_r.at[p], partner) for p in range(AG_PIECES)]

    def gated(gate, up):
        return (gate * jax.nn.sigmoid(gate) * up).astype(BF16)

    def local_ffn(i):
        rows = rows_buf[pl.ds(0, 2 * ROWS), :]
        gate, up = [jnp.dot(rows, wint_buf[i, part, :, :widths[i]], preferred_element_type=F32) for part in range(2)]
        g_buf[pl.ds(0, 2 * ROWS), pl.ds(i * F_CHUNK, widths[i])] = gated(gate, up)

    def ahead_chunk(i, phase):
        k0, size = K_PARTS[phase]
        rows = rows_buf[pl.ds(2 * ROWS, 2 * ROWS), k0:k0 + size]
        cols = pl.ds(i * F_CHUNK, widths[i])
        sums = []
        for part in range(2):
            prod = jnp.dot(rows, wint_buf[i, part, k0:k0 + size, :], preferred_element_type=F32)
            sums.append(prod if phase == 0 else part_acc[part, :, cols] + prod)
        if phase < len(K_PARTS) - 1:
            for part in range(2):
                part_acc[part, :, cols] = sums[part]
        else:
            g_buf[pl.ds(2 * ROWS, 2 * ROWS), cols] = gated(sums[0], sums[1])

    def late_chunk(i, phase):
        k0, size = K_PARTS[phase]
        rows = rows_buf[:, k0:k0 + size]
        cols = pl.ds((i - N_T) * F_CHUNK, widths[i])
        sums = []
        for part in range(2):
            prod = lax.dot_general(rows, win_buf[i % RING, part, :widths[i], k0:k0 + size],
                                   (((1,), (1,)), ((), ())), preferred_element_type=F32)
            sums.append(prod if phase == 0 else late_acc[part, :, cols] + prod)
        if phase < len(K_PARTS) - 1:
            for part in range(2):
                late_acc[part, :, cols] = sums[part]
        else:
            g_buf[:, pl.ds(i * F_CHUNK, widths[i])] = gated(sums[0], sums[1])

    def remote_phase(phase, first, last):
        for i in range(first, last):
            (ahead_chunk if i < N_T else late_chunk)(i, phase)

    def relay(p):
        cross_copies[p].wait_recv()
        relays[p].start()

    for i in range(N_T):
        if i == 1:
            pair_copy.wait()
        win_copy(i, widths[i]).wait()
        for part in range(2):
            wint_buf[i, part] = win_buf[i % RING, part].T
        if i + RING < N_F:
            win_copy(i + RING, widths[i + RING]).start(priority=1)
        else:
            wout_copy(i + RING - N_F).start(priority=1)
        if i >= 1:
            local_ffn(i - 1)
        if i in RELAY_AT:
            relay(RELAY_AT.index(i))
    for j in range(N_T + RING - N_F, N_W):
        wout_copy(j).start(priority=1)
    local_ffn(N_T - 1)
    for i in range(N_T, N_F):
        win_copy(i, widths[i]).wait()
    if len(RELAY_AT) < 3:
        relay(2)
    for p in range(2):
        relays[p].wait_recv()
    remote_phase(0, 0, CUT)
    relay(3)
    remote_phase(0, CUT, N_F)
    relays[2].wait_recv()
    relays[3].wait_recv()
    remote_phase(1, 0, N_F)
    for p in range(AG_PIECES):
        cross_copies[p].wait_send()
        relays[p].wait_send()
    for j in range(N_W):
        wout_copy(j).wait()
    h_copy.wait()

    def piece(k):
        return pl.ds(D_EDGES[k], D_EDGES[k + 1] - D_EDGES[k])

    def block_send(src, dst, ssem, rsem, peer):
        return [send(src.at[:, piece(k)], dst.at[:, piece(k)], ssem.at[k], rsem.at[k], peer) for k in range(N_D)]

    pair_copies = block_send(pair_send, pair_recv, ps_s, ps_r, partner)
    near_copies = block_send(near_send, near_recv, ns_s, ns_r, partner)
    far_copies = block_send(far_send, far_recv, fs_s, fs_r, cross)

    def remote_block(k):
        part = jnp.dot(g_buf[2 * ROWS:, :], wout_buf[:, piece(k)], preferred_element_type=F32)
        far_keep[:, piece(k)] = part[:ROWS]
        pair_send[:, piece(k)] = part[ROWS:].astype(BF16)
        pair_copies[k].start()

    def local_block(k):
        part = jnp.dot(g_buf[:2 * ROWS, :], wout_buf[:, piece(k)], preferred_element_type=F32)
        own_acc[:, piece(k)] = part[:ROWS] + h_ref[:, piece(k)]
        near_send[:, piece(k)] = part[ROWS:].astype(BF16)
        near_copies[k].start()

    def pair_sum(k):
        pair_copies[k].wait_recv()
        far_send[:, piece(k)] = (far_keep[:, piece(k)] + pair_recv[:, piece(k)].astype(F32)).astype(BF16)
        far_copies[k].start()

    steps = [(remote_block, k) for k in range(N_D)] + [(local_block, k) for k in range(N_D)]
    for n, (step, k) in enumerate(steps):
        step(k)
        if 0 <= n - PAIR_LAG < N_D:
            pair_sum(n - PAIR_LAG)
    for k in range(N_D):
        near_copies[k].wait_recv()
        far_copies[k].wait_recv()
        y_ref[:, piece(k)] = (own_acc[:, piece(k)] + near_recv[:, piece(k)].astype(F32)
                              + far_recv[:, piece(k)].astype(F32)).astype(BF16)
    for k in range(N_D):
        pair_copies[k].wait_send()
        near_copies[k].wait_send()
        far_copies[k].wait_send()


def mlp(m, h, w_in, w_out):
    vmem = pl.BlockSpec(memory_space=pltpu.VMEM)
    hbm = pl.BlockSpec(memory_space=pl.ANY)
    dma = pltpu.SemaphoreType.DMA
    piece = (ROWS, HIDDEN)
    return pl.pallas_call(
        mlp_kernel,
        out_shape=jax.ShapeDtypeStruct((ROWS, HIDDEN), BF16),
        in_specs=[hbm] * 4,
        out_specs=vmem,
        scratch_shapes=[
            pltpu.VMEM((ROWS, HIDDEN), BF16), pltpu.VMEM((ROWS, HIDDEN), F32),
            pltpu.VMEM((4 * ROWS, HIDDEN), BF16),
            pltpu.VMEM((2, 2 * ROWS, N_T * F_CHUNK), F32),
            pltpu.VMEM((2, 4 * ROWS, (N_F - N_T) * F_CHUNK), F32),
            pltpu.VMEM((RING, 2, F_CHUNK, HIDDEN), BF16),
            pltpu.VMEM((N_T, 2, HIDDEN, F_CHUNK), BF16),
            pltpu.VMEM((FFN_LOC, HIDDEN), BF16),
            pltpu.VMEM((4 * ROWS, FFN_LOC), BF16),
            pltpu.VMEM(piece, BF16), pltpu.VMEM(piece, BF16),
            pltpu.VMEM(piece, BF16), pltpu.VMEM(piece, BF16),
            pltpu.VMEM(piece, F32), pltpu.VMEM(piece, BF16), pltpu.VMEM(piece, BF16),
            pltpu.VMEM(piece, F32),
            dma((2,)), dma((RING,)), dma((N_W,)),
            dma((AG_PIECES,)), dma((AG_PIECES,)), dma, dma, dma((AG_PIECES,)), dma((AG_PIECES,)),
            dma((N_D,)), dma((N_D,)), dma((N_D,)), dma((N_D,)), dma((N_D,)), dma((N_D,)),
        ],
        compiler_params=pltpu.CompilerParams(vmem_limit_bytes=50 * 1024 * 1024, collective_id=0, has_side_effects=True),
        name="mlp_block",
    )(m, h, w_in, w_out)


def rope_freq():
    pair = 2 * (np.arange(HEAD_DIM) // 2)
    return jnp.asarray((ROPE_BASE ** (-pair / (HEAD_DIM // 2)))[None, :], F32)


def solution(mesh):
    row_spec = P(('rep', 'grp'))
    repl_spec = P()

    def local_layer(x_in, seq_len, k_cache, v_cache, gamma_attn, w_qkv, b_qkv, w_proj, gamma_mlp, w_in, w_out):
        k_flat = k_cache.reshape(ROWS, FLAT, HEAD_DIM)
        v_flat = v_cache.reshape(ROWS, FLAT, HEAD_DIM)
        h, m, k_out, v_out = attention(seq_len, rope_freq(), x_in, gamma_attn, gamma_mlp, b_qkv, w_qkv, k_flat, v_flat, w_proj)
        layer_out = mlp(m, h, w_in, w_out)
        return layer_out, k_out.reshape(k_cache.shape), v_out.reshape(v_cache.shape)

    return jax.shard_map(local_layer, mesh=mesh,
                         in_specs=(row_spec, row_spec, row_spec, row_spec, repl_spec, repl_spec, repl_spec,
                                   repl_spec, repl_spec, P(None, 'grp', None), P('grp', None)),
                         out_specs=(row_spec, row_spec, row_spec), check_vma=False)
```

```python
import jax
import jax.numpy as jnp
import numpy as np
from jax import lax
from jax.experimental import pallas as pl
from jax.experimental.pallas import tpu as pltpu
from jax.sharding import PartitionSpec as P

HEAD_DIM = 128
ROPE_BASE = 10000.0
EPS = 1e-5
HIDDEN = 2048
HEADS = 16
KV = 2
ROWS = 64
LMAX = 256
FLAT = LMAX * KV
FFN_LOC = 2752
QKV_CHUNK = 512
N_QKV = 5
PROJ_CHUNK = 512
N_PROJ = 4
SEQ_CHUNK = 8
N_SEQ = ROWS // SEQ_CHUNK
WINDOW = 7
OUT_LAG = 4
F_CHUNK = 256
N_F = 11
DIRECT = 256
D_EDGES = (0, 512, 1024, 1536, 2048)
N_D = len(D_EDGES) - 1
PAIR_LAG = 2
AG_PIECES = 4
AG_COLS = HIDDEN // AG_PIECES
K_PARTS = ((0, HIDDEN // 2), (HIDDEN // 2, HIDDEN // 2))
RING = 4
CUT = 6
N_T = 9
N_W = 4
W_ROWS = FFN_LOC // N_W
RELAY_AT = (5, 7)
HBM_ROWS = 2048
F32 = jnp.float32
BF16 = jnp.bfloat16


def attn_kernel(len_ref, freq_hbm, x_hbm, ga_hbm, gm_hbm, b_hbm, wqkv_hbm, k_hbm, v_hbm, wproj_hbm,
                h_hbm, m_hbm, kout_hbm, vout_hbm,
                freq_ref, x_ref, ga_ref, gm_ref, b_ref, h_ref, m_ref,
                wq_buf, wp_buf, k_buf, v_buf, q_scr, kn_scr, vn_scr, ctx_scr, act_buf,
                small_sem, wq_sem, wp_sem, k_sem, v_sem, out_sem):
    small = [pltpu.make_async_copy(src, dst, small_sem.at[n]) for n, (src, dst) in enumerate(
        ((x_hbm, x_ref), (ga_hbm, ga_ref), (freq_hbm, freq_ref), (b_hbm, b_ref), (gm_hbm, gm_ref)))]

    def wq_copy(c):
        return pltpu.make_async_copy(wqkv_hbm.at[:, pl.ds(c * QKV_CHUNK, QKV_CHUNK)], wq_buf.at[c], wq_sem.at[c])

    def wp_copy(c):
        return pltpu.make_async_copy(wproj_hbm.at[:, pl.ds(c * PROJ_CHUNK, PROJ_CHUNK)], wp_buf.at[c], wp_sem.at[c])

    def k_copy(i):
        rows = pl.ds(i * SEQ_CHUNK, SEQ_CHUNK)
        return pltpu.make_async_copy(k_hbm.at[rows], k_buf.at[rows], k_sem.at[i])

    def v_copy(i):
        rows = pl.ds(i * SEQ_CHUNK, SEQ_CHUNK)
        return pltpu.make_async_copy(v_hbm.at[rows], v_buf.at[rows], v_sem.at[i])

    def ko_copy(i):
        rows = pl.ds(i * SEQ_CHUNK, SEQ_CHUNK)
        return pltpu.make_async_copy(k_buf.at[rows], kout_hbm.at[rows], k_sem.at[i])

    def vo_copy(i):
        rows = pl.ds(i * SEQ_CHUNK, SEQ_CHUNK)
        return pltpu.make_async_copy(v_buf.at[rows], vout_hbm.at[rows], v_sem.at[i])

    for cp in small:
        cp.start()
    def fetch(n):
        if n < N_QKV:
            wq_copy(n).start()
        elif n < N_QKV + N_SEQ:
            k_copy(n - N_QKV).start()
            v_copy(n - N_QKV).start()
        elif n < N_QKV + N_SEQ + N_PROJ:
            wp_copy(n - N_QKV - N_SEQ).start()

    for n in range(WINDOW):
        fetch(n)

    for cp in small:
        cp.wait()
    x = x_ref[...].astype(F32)
    inv = lax.rsqrt(jnp.mean(x * x, axis=-1, keepdims=True) + EPS)
    act_buf[...] = (x * inv * ga_ref[...].astype(F32).reshape(1, HIDDEN)).astype(BF16)
    normed = act_buf[...]
    sub = lax.broadcasted_iota(jnp.int32, (8, HEAD_DIM), 0)
    tiles = []
    for t in range(ROWS // 8):
        tile = jnp.zeros((8, HEAD_DIM), jnp.int32)
        for r in range(8):
            tile = jnp.where(sub == r, len_ref[t * 8 + r], tile)
        tiles.append(tile)
    angles = jnp.concatenate(tiles, axis=0).astype(F32) * freq_ref[...]
    lane = lax.broadcasted_iota(jnp.int32, (ROWS, HEAD_DIM), 1)
    even = (lane % 2) == 0
    turned = lane < HEAD_DIM // 2
    cosine = jnp.where(turned, jnp.cos(angles), 1.0)
    sine = jnp.sin(angles)
    sine = jnp.where(turned, jnp.where(even, -sine, sine), 0.0)
    bias = b_ref[...].astype(F32).reshape(1, HIDDEN + 2 * KV * HEAD_DIM)

    def rotate(v):
        swapped = jnp.where(even, pltpu.roll(v, HEAD_DIM - 1, 1), pltpu.roll(v, 1, 1))
        return v * cosine + swapped * sine

    for c in range(N_QKV):
        wq_copy(c).wait()
        fetch(c + WINDOW)
        acc = jnp.dot(normed, wq_buf[c], preferred_element_type=F32) + bias[:, c * QKV_CHUNK:(c + 1) * QKV_CHUNK]
        for t in range(QKV_CHUNK // HEAD_DIM):
            head = c * (QKV_CHUNK // HEAD_DIM) + t
            part = acc[:, t * HEAD_DIM:(t + 1) * HEAD_DIM]
            if head < HEADS:
                q_scr[pl.ds(head, ROWS, stride=HEADS), :] = rotate(part)
            elif head < HEADS + KV:
                kn_scr[head - HEADS] = rotate(part)
            else:
                vn_scr[head - HEADS - KV] = part

    row16 = lax.broadcasted_iota(jnp.int32, (16, HEAD_DIM), 0)
    col = lax.broadcasted_iota(jnp.int32, (HEADS, FLAT), 1)
    row32 = lax.broadcasted_iota(jnp.int32, (2 * HEADS, HEAD_DIM), 0)
    head_row = lax.broadcasted_iota(jnp.int32, (HEADS, FLAT), 0)
    pos = jnp.where((col % KV) == (head_row // (HEADS // KV)), col // KV, 2 * LMAX)

    def insert(i):
        for u in range(SEQ_CHUNK):
            b = i * SEQ_CHUNK + u
            ln = len_ref[b]
            base = pl.multiple_of((ln // 8) * 16, 16)
            hit = (row16 // 2) == (ln % 8)
            for buf, new in ((k_buf, kn_scr), (v_buf, vn_scr)):
                fresh = jnp.where(row16 % 2 == 0, new[0, pl.ds(b, 1), :], new[1, pl.ds(b, 1), :])
                old = buf[b, pl.ds(base, 16), :].astype(F32)
                buf[b, pl.ds(base, 16), :] = jnp.where(hit, fresh, old).astype(BF16)

    def scores(i):
        out = []
        for u in range(0, SEQ_CHUNK, 2):
            b = i * SEQ_CHUNK + u
            q = q_scr[pl.ds(b * HEADS, 2 * HEADS), :]
            first = row32 < HEADS
            q2 = jnp.concatenate([jnp.where(first, q, 0.0), jnp.where(first, 0.0, q)], axis=1).astype(BF16)
            k2 = jnp.concatenate([k_buf[b], k_buf[b + 1]], axis=1)
            out.append(lax.dot_general(q2, k2, (((1,), (1,)), ((), ())), preferred_element_type=F32))
        return out

    def probabilities(i, raw):
        probs = []
        for u in range(0, SEQ_CHUNK, 2):
            b = i * SEQ_CHUNK + u
            s2 = raw[u // 2]
            pair = []
            for t in range(2):
                s = jnp.where(pos <= len_ref[b + t], s2[t * HEADS:(t + 1) * HEADS], -jnp.inf)
                e = jnp.exp((s - jnp.max(s, axis=1, keepdims=True)) * (HEAD_DIM ** -0.5))
                pair.append((e * (1.0 / jnp.sum(e, axis=1, keepdims=True))).astype(BF16))
            probs.append(jnp.concatenate(pair, axis=0))
        return probs

    def weighted_values(i, probs):
        for u in range(0, SEQ_CHUNK, 2):
            b = i * SEQ_CHUNK + u
            v2 = jnp.concatenate([v_buf[b], v_buf[b + 1]], axis=1)
            c2 = jnp.dot(probs[u // 2], v2, preferred_element_type=F32)
            ctx_scr[pl.ds(b * HEADS, HEADS), :] = c2[:HEADS, :HEAD_DIM]
            ctx_scr[pl.ds((b + 1) * HEADS, HEADS), :] = c2[HEADS:, HEAD_DIM:]

    probs = None
    for i in range(N_SEQ):
        k_copy(i).wait()
        v_copy(i).wait()
        fetch(N_QKV + i + WINDOW)
        if i >= OUT_LAG:
            ko_copy(i - OUT_LAG).start()
            vo_copy(i - OUT_LAG).start()
        insert(i)
        raw = scores(i)
        if i > 0:
            weighted_values(i - 1, probs)
        probs = probabilities(i, raw)
    for i in range(N_SEQ - OUT_LAG, N_SEQ):
        ko_copy(i).start()
        vo_copy(i).start()
    weighted_values(N_SEQ - 1, probs)

    for h in range(HEADS):
        act_buf[:, h * HEAD_DIM:(h + 1) * HEAD_DIM] = ctx_scr[pl.ds(h, ROWS, stride=HEADS), :].astype(BF16)
    ctx = act_buf[...]
    total = jnp.zeros((ROWS, 1), F32)
    for c in range(N_PROJ):
        wp_copy(c).wait()
        cols = slice(c * PROJ_CHUNK, (c + 1) * PROJ_CHUNK)
        hid = x_ref[:, cols].astype(F32) + jnp.dot(ctx, wp_buf[c], preferred_element_type=F32)
        h_ref[:, cols] = hid
        total = total + jnp.sum(hid * hid, axis=-1, keepdims=True)
    inv2 = lax.rsqrt(total * (1.0 / HIDDEN) + EPS)
    m_ref[...] = (h_ref[...] * inv2 * gm_ref[...].astype(F32).reshape(1, HIDDEN)).astype(BF16)
    h_copy = pltpu.make_async_copy(h_ref, h_hbm.at[pl.ds(0, ROWS)], out_sem.at[0])
    m_copy = pltpu.make_async_copy(m_ref, m_hbm.at[pl.ds(0, ROWS)], out_sem.at[1])
    h_copy.start()
    m_copy.start()
    for i in range(N_SEQ):
        ko_copy(i).wait()
        vo_copy(i).wait()
    h_copy.wait()
    m_copy.wait()


def attention(lens, freq, x, ga, gm, bias, w_qkv, k_flat, v_flat, w_proj):
    hbm = pl.BlockSpec(memory_space=pl.ANY)
    smem = pl.BlockSpec(memory_space=pltpu.SMEM)
    dma = pltpu.SemaphoreType.DMA
    return pl.pallas_call(
        attn_kernel,
        out_shape=(jax.ShapeDtypeStruct((HBM_ROWS, HIDDEN), F32), jax.ShapeDtypeStruct((HBM_ROWS, HIDDEN), BF16),
                   jax.ShapeDtypeStruct(k_flat.shape, BF16), jax.ShapeDtypeStruct(v_flat.shape, BF16)),
        in_specs=[smem] + [hbm] * 9,
        out_specs=(hbm,) * 4,
        scratch_shapes=[
            pltpu.VMEM((1, HEAD_DIM), F32), pltpu.VMEM((ROWS, HIDDEN), BF16), pltpu.VMEM((HIDDEN,), BF16),
            pltpu.VMEM((HIDDEN,), BF16), pltpu.VMEM((HIDDEN + 2 * KV * HEAD_DIM,), BF16),
            pltpu.VMEM((ROWS, HIDDEN), F32), pltpu.VMEM((ROWS, HIDDEN), BF16),
            pltpu.VMEM((N_QKV, HIDDEN, QKV_CHUNK), BF16),
            pltpu.VMEM((N_PROJ, HIDDEN, PROJ_CHUNK), BF16),
            pltpu.VMEM((ROWS, FLAT, HEAD_DIM), BF16),
            pltpu.VMEM((ROWS, FLAT, HEAD_DIM), BF16),
            pltpu.VMEM((ROWS * HEADS, HEAD_DIM), F32),
            pltpu.VMEM((KV, ROWS, HEAD_DIM), F32),
            pltpu.VMEM((KV, ROWS, HEAD_DIM), F32),
            pltpu.VMEM((ROWS * HEADS, HEAD_DIM), F32),
            pltpu.VMEM((ROWS, HIDDEN), BF16),
            dma((5,)), dma((N_QKV,)), dma((N_PROJ,)), dma((N_SEQ,)), dma((N_SEQ,)), dma((2,)),
        ],
        compiler_params=pltpu.CompilerParams(vmem_limit_bytes=60 * 1024 * 1024),
        name="attn_block",
    )(lens, freq, x, ga, gm, bias, w_qkv, k_flat, v_flat, w_proj)


def mlp_kernel(m_hbm, h_hbm, win_hbm, wout_hbm, y_ref,
               m_ref, h_ref, rows_buf, part_acc, late_acc, win_buf, wint_buf, wout_buf, g_buf, pair_send, pair_recv, near_send, near_recv, far_keep, far_send, far_recv,
               own_acc, direct_send, direct_recv, in_sem, win_sem, wout_sem, agx_s, agx_r, agp_s, agp_r, agr_s, agr_r,
               ps_s, ps_r, ns_s, ns_r, fs_s, fs_r, ds_s, ds_r):
    me = lax.axis_index('grp')
    partner = me + 1 - 2 * (me % 2)
    cross = (me + 2) % 4
    diag = (partner + 2) % 4

    def win_copy(i, width):
        src = win_hbm.at[:, pl.ds(i * F_CHUNK, width)]
        return pltpu.make_async_copy(src, win_buf.at[i % RING, :, pl.ds(0, width)], win_sem.at[i % RING])

    def wout_copy(j):
        rows = pl.ds(j * W_ROWS, W_ROWS)
        return pltpu.make_async_copy(wout_hbm.at[rows], wout_buf.at[rows], wout_sem.at[j])

    m_copy = pltpu.make_async_copy(m_hbm.at[pl.ds(0, ROWS)], m_ref, in_sem.at[0])
    h_copy = pltpu.make_async_copy(h_hbm.at[pl.ds(0, ROWS)], h_ref, in_sem.at[1])
    m_copy.start()
    tail = FFN_LOC - (N_F - 1) * F_CHUNK
    widths = [F_CHUNK] * (N_F - 1) + [tail]
    first_copies = [pltpu.make_async_copy(win_hbm.at[part, pl.ds(0, F_CHUNK)], win_buf.at[0, part],
                                          win_sem.at[part * RING]) for part in range(2)]
    for cp in first_copies:
        cp.start(priority=1)
    for i in range(1, RING):
        win_copy(i, widths[i]).start(priority=1)
    h_copy.start()

    barrier = pltpu.get_barrier_semaphore()
    for peer in (partner, cross, diag):
        pl.semaphore_signal(barrier, inc=1, device_id={'grp': peer}, device_id_type=pl.DeviceIdType.MESH)
    pl.semaphore_wait(barrier, 3)

    def send(src, dst, ssem, rsem, peer):
        return pltpu.make_async_remote_copy(src_ref=src, dst_ref=dst, send_sem=ssem, recv_sem=rsem,
                                            device_id={'grp': peer}, device_id_type=pl.DeviceIdType.MESH)

    def part_of(slot, p):
        return rows_buf.at[pl.ds(slot * ROWS, ROWS), pl.ds(p * AG_COLS, AG_COLS)]

    cross_copies = [send(m_ref.at[:, pl.ds(p * AG_COLS, AG_COLS)], part_of(2, p), agx_s.at[p], agx_r.at[p], cross)
                    for p in range(AG_PIECES)]
    m_copy.wait()
    for cp in cross_copies:
        cp.start()
    pair_copy = send(m_ref, rows_buf.at[pl.ds(ROWS, ROWS)], agp_s, agp_r, partner)
    pair_copy.start()
    rows_buf[pl.ds(0, ROWS), :] = m_ref[...]
    relays = [send(part_of(2, p), part_of(3, p), agr_s.at[p], agr_r.at[p], partner) for p in range(AG_PIECES)]

    def gated(gate, up):
        return (gate * jax.nn.sigmoid(gate) * up).astype(BF16)

    def local_ffn(i):
        rows = rows_buf[pl.ds(0, 2 * ROWS), :]
        gate, up = [jnp.dot(rows, wint_buf[i, part, :, :widths[i]], preferred_element_type=F32) for part in range(2)]
        g_buf[pl.ds(0, 2 * ROWS), pl.ds(i * F_CHUNK, widths[i])] = gated(gate, up)

    def ahead_chunk(i, phase):
        k0, size = K_PARTS[phase]
        rows = rows_buf[pl.ds(2 * ROWS, 2 * ROWS), k0:k0 + size]
        cols = pl.ds(i * F_CHUNK, widths[i])
        sums = []
        for part in range(2):
            prod = jnp.dot(rows, wint_buf[i, part, k0:k0 + size, :], preferred_element_type=F32)
            sums.append(prod if phase == 0 else part_acc[part, :, cols] + prod)
        if phase < len(K_PARTS) - 1:
            for part in range(2):
                part_acc[part, :, cols] = sums[part]
        else:
            g_buf[pl.ds(2 * ROWS, 2 * ROWS), cols] = gated(sums[0], sums[1])

    def late_chunk(i, phase):
        k0, size = K_PARTS[phase]
        rows = rows_buf[:, k0:k0 + size]
        cols = pl.ds((i - N_T) * F_CHUNK, widths[i])
        sums = []
        for part in range(2):
            prod = lax.dot_general(rows, win_buf[i % RING, part, :widths[i], k0:k0 + size],
                                   (((1,), (1,)), ((), ())), preferred_element_type=F32)
            sums.append(prod if phase == 0 else late_acc[part, :, cols] + prod)
        if phase < len(K_PARTS) - 1:
            for part in range(2):
                late_acc[part, :, cols] = sums[part]
        else:
            g_buf[:, pl.ds(i * F_CHUNK, widths[i])] = gated(sums[0], sums[1])

    def remote_phase(phase, first, last):
        for i in range(first, last):
            (ahead_chunk if i < N_T else late_chunk)(i, phase)

    def relay(p):
        cross_copies[p].wait_recv()
        relays[p].start()

    for i in range(N_T):
        if i == 1:
            pair_copy.wait()
        if i > 0:
            win_copy(i, widths[i]).wait()
        for part in range(2):
            if i == 0:
                first_copies[part].wait()
            wint_buf[i, part] = win_buf[i % RING, part].T
        if i + RING < N_F:
            win_copy(i + RING, widths[i + RING]).start(priority=1)
        else:
            wout_copy(i + RING - N_F).start(priority=1)
        if i >= 1:
            local_ffn(i - 1)
        if i in RELAY_AT:
            relay(RELAY_AT.index(i))
    for j in range(N_T + RING - N_F, N_W):
        wout_copy(j).start(priority=1)
    local_ffn(N_T - 1)
    for i in range(N_T, N_F):
        win_copy(i, widths[i]).wait()
    if len(RELAY_AT) < 3:
        relay(2)
    for p in range(2):
        relays[p].wait_recv()
    remote_phase(0, 0, CUT)
    relay(3)
    remote_phase(0, CUT, N_F)
    relays[2].wait_recv()
    relays[3].wait_recv()
    remote_phase(1, 0, N_F)
    for p in range(AG_PIECES):
        cross_copies[p].wait_send()
        relays[p].wait_send()
    for j in range(N_W):
        wout_copy(j).wait()
    h_copy.wait()

    def piece(k, shared=False):
        start = max(D_EDGES[k], DIRECT) if shared else D_EDGES[k]
        return pl.ds(start, D_EDGES[k + 1] - start)

    def block_send(src, dst, ssem, rsem, peer, shared=True):
        return [send(src.at[:, piece(k, shared)], dst.at[:, piece(k, shared)], ssem.at[k], rsem.at[k], peer) for k in range(N_D)]

    pair_copies = block_send(pair_send, pair_recv, ps_s, ps_r, partner)
    near_copies = block_send(near_send, near_recv, ns_s, ns_r, partner, shared=False)
    far_copies = block_send(far_send, far_recv, fs_s, fs_r, cross)

    direct_copies = [send(direct_send.at[pl.ds(n * ROWS, ROWS)], direct_recv.at[pl.ds(n * ROWS, ROWS)],
                          ds_s.at[n], ds_r.at[n], (cross, diag)[n]) for n in range(2)]

    def down(rows, k):
        return jnp.dot(g_buf[rows, :], wout_buf[:, piece(k)], preferred_element_type=F32)

    def remote_block(k):
        part = down(slice(2 * ROWS, 4 * ROWS), k)
        if k == 0:
            direct_send[...] = part[:, :DIRECT].astype(BF16)
            for cp in direct_copies:
                cp.start()
            part = part[:, DIRECT:]
        far_keep[:, piece(k, True)] = part[:ROWS]
        pair_send[:, piece(k, True)] = part[ROWS:].astype(BF16)
        pair_copies[k].start()

    def local_block(k):
        part = down(slice(0, 2 * ROWS), k)
        own_acc[:, piece(k)] = part[:ROWS] + h_ref[:, piece(k)]
        near_send[:, piece(k)] = part[ROWS:].astype(BF16)
        near_copies[k].start()

    def pair_sum(k):
        cols = piece(k, True)
        pair_copies[k].wait_recv()
        far_send[:, cols] = (far_keep[:, cols] + pair_recv[:, cols].astype(F32)).astype(BF16)
        far_copies[k].start()

    steps = [(remote_block, k) for k in range(N_D)] + [(local_block, k) for k in range(N_D)]
    for n, (step, k) in enumerate(steps):
        step(k)
        if 0 <= n - PAIR_LAG < N_D:
            pair_sum(n - PAIR_LAG)
    for cp in direct_copies:
        cp.wait()
    for k in range(N_D):
        near_copies[k].wait_recv()
        near = own_acc[:, piece(k)] + near_recv[:, piece(k)].astype(F32)
        if k == 0:
            direct = direct_recv[...].astype(F32)
            y_ref[:, :DIRECT] = (near[:, :DIRECT] + direct[:ROWS] + direct[ROWS:]).astype(BF16)
            near = near[:, DIRECT:]
        far_copies[k].wait_recv()
        y_ref[:, piece(k, True)] = (near + far_recv[:, piece(k, True)].astype(F32)).astype(BF16)
    for k in range(N_D):
        pair_copies[k].wait_send()
        near_copies[k].wait_send()
        far_copies[k].wait_send()


def mlp(m, h, w_in, w_out):
    vmem = pl.BlockSpec(memory_space=pltpu.VMEM)
    hbm = pl.BlockSpec(memory_space=pl.ANY)
    dma = pltpu.SemaphoreType.DMA
    piece = (ROWS, HIDDEN)
    return pl.pallas_call(
        mlp_kernel,
        out_shape=jax.ShapeDtypeStruct((ROWS, HIDDEN), BF16),
        in_specs=[hbm] * 4,
        out_specs=vmem,
        scratch_shapes=[
            pltpu.VMEM((ROWS, HIDDEN), BF16), pltpu.VMEM((ROWS, HIDDEN), F32),
            pltpu.VMEM((4 * ROWS, HIDDEN), BF16),
            pltpu.VMEM((2, 2 * ROWS, N_T * F_CHUNK), F32),
            pltpu.VMEM((2, 4 * ROWS, (N_F - N_T) * F_CHUNK), F32),
            pltpu.VMEM((RING, 2, F_CHUNK, HIDDEN), BF16),
            pltpu.VMEM((N_T, 2, HIDDEN, F_CHUNK), BF16),
            pltpu.VMEM((FFN_LOC, HIDDEN), BF16),
            pltpu.VMEM((4 * ROWS, FFN_LOC), BF16),
            pltpu.VMEM(piece, BF16), pltpu.VMEM(piece, BF16),
            pltpu.VMEM(piece, BF16), pltpu.VMEM(piece, BF16),
            pltpu.VMEM(piece, F32), pltpu.VMEM(piece, BF16), pltpu.VMEM(piece, BF16),
            pltpu.VMEM(piece, F32),
            pltpu.VMEM((2 * ROWS, DIRECT), BF16), pltpu.VMEM((2 * ROWS, DIRECT), BF16),
            dma((2,)), dma((RING + 1,)), dma((N_W,)),
            dma((AG_PIECES,)), dma((AG_PIECES,)), dma, dma, dma((AG_PIECES,)), dma((AG_PIECES,)),
            dma((N_D,)), dma((N_D,)), dma((N_D,)), dma((N_D,)), dma((N_D,)), dma((N_D,)), dma((2,)), dma((2,)),
        ],
        compiler_params=pltpu.CompilerParams(vmem_limit_bytes=50 * 1024 * 1024, collective_id=0, has_side_effects=True),
        name="mlp_block",
    )(m, h, w_in, w_out)


def rope_freq():
    pair = 2 * (np.arange(HEAD_DIM) // 2)
    return jnp.asarray((ROPE_BASE ** (-pair / (HEAD_DIM // 2)))[None, :], F32)


def solution(mesh):
    row_spec = P(('rep', 'grp'))
    repl_spec = P()

    def local_layer(x_in, seq_len, k_cache, v_cache, gamma_attn, w_qkv, b_qkv, w_proj, gamma_mlp, w_in, w_out):
        k_flat = k_cache.reshape(ROWS, FLAT, HEAD_DIM)
        v_flat = v_cache.reshape(ROWS, FLAT, HEAD_DIM)
        h, m, k_out, v_out = attention(seq_len, rope_freq(), x_in, gamma_attn, gamma_mlp, b_qkv, w_qkv, k_flat, v_flat, w_proj)
        layer_out = mlp(m, h, w_in, w_out)
        return layer_out, k_out.reshape(k_cache.shape), v_out.reshape(v_cache.shape)

    return jax.shard_map(local_layer, mesh=mesh,
                         in_specs=(row_spec, row_spec, row_spec, row_spec, repl_spec, repl_spec, repl_spec,
                                   repl_spec, repl_spec, P(None, 'grp', None), P('grp', None)),
                         out_specs=(row_spec, row_spec, row_spec), check_vma=False)
```

```python
import jax
import jax.numpy as jnp
import numpy as np
from jax import lax
from jax.experimental import pallas as pl
from jax.experimental.pallas import tpu as pltpu
from jax.sharding import PartitionSpec as P

HEAD_DIM = 128
ROPE_BASE = 10000.0
EPS = 1e-5
HIDDEN = 2048
HEADS = 16
KV = 2
ROWS = 64
LMAX = 256
FLAT = LMAX * KV
FFN_LOC = 2752
QKV_CHUNK = 512
N_QKV = 5
PROJ_CHUNK = 512
N_PROJ = 4
SEQ_CHUNK = 8
N_SEQ = ROWS // SEQ_CHUNK
WINDOW = 7
OUT_LAG = 4
F_CHUNK = 256
N_F = 11
DIRECT = 256
D_EDGES = (0, 512, 1024, 1536, 2048)
N_D = len(D_EDGES) - 1
PAIR_LAG = 2
AG_PIECES = 4
AG_COLS = HIDDEN // AG_PIECES
K_PARTS = ((0, HIDDEN // 2), (HIDDEN // 2, HIDDEN // 2))
RING = 4
CUT = 4
N_T = 9
N_W = 4
W_ROWS = FFN_LOC // N_W
RELAY_AT = (4, 6)
HBM_ROWS = 2048
F32 = jnp.float32
BF16 = jnp.bfloat16


def attn_kernel(len_ref, freq_hbm, x_hbm, ga_hbm, gm_hbm, b_hbm, wqkv_hbm, k_hbm, v_hbm, wproj_hbm,
                h_hbm, m_hbm, kout_hbm, vout_hbm,
                freq_ref, x_ref, ga_ref, gm_ref, b_ref, h_ref, m_ref,
                wq_buf, wp_buf, k_buf, v_buf, q_scr, kn_scr, vn_scr, ctx_scr, act_buf,
                small_sem, wq_sem, wp_sem, k_sem, v_sem, out_sem):
    small = [pltpu.make_async_copy(src, dst, small_sem.at[n]) for n, (src, dst) in enumerate(
        ((x_hbm, x_ref), (ga_hbm, ga_ref), (freq_hbm, freq_ref), (b_hbm, b_ref), (gm_hbm, gm_ref)))]

    def wq_copy(c):
        return pltpu.make_async_copy(wqkv_hbm.at[:, pl.ds(c * QKV_CHUNK, QKV_CHUNK)], wq_buf.at[c], wq_sem.at[c])

    def wp_copy(c):
        return pltpu.make_async_copy(wproj_hbm.at[:, pl.ds(c * PROJ_CHUNK, PROJ_CHUNK)], wp_buf.at[c], wp_sem.at[c])

    def k_copy(i):
        rows = pl.ds(i * SEQ_CHUNK, SEQ_CHUNK)
        return pltpu.make_async_copy(k_hbm.at[rows], k_buf.at[rows], k_sem.at[i])

    def v_copy(i):
        rows = pl.ds(i * SEQ_CHUNK, SEQ_CHUNK)
        return pltpu.make_async_copy(v_hbm.at[rows], v_buf.at[rows], v_sem.at[i])

    def ko_copy(i):
        rows = pl.ds(i * SEQ_CHUNK, SEQ_CHUNK)
        return pltpu.make_async_copy(k_buf.at[rows], kout_hbm.at[rows], k_sem.at[i])

    def vo_copy(i):
        rows = pl.ds(i * SEQ_CHUNK, SEQ_CHUNK)
        return pltpu.make_async_copy(v_buf.at[rows], vout_hbm.at[rows], v_sem.at[i])

    for cp in small:
        cp.start()
    def fetch(n):
        if n < N_QKV:
            wq_copy(n).start()
        elif n < N_QKV + N_SEQ:
            k_copy(n - N_QKV).start()
            v_copy(n - N_QKV).start()
        elif n < N_QKV + N_SEQ + N_PROJ:
            wp_copy(n - N_QKV - N_SEQ).start()

    for n in range(WINDOW):
        fetch(n)

    for cp in small:
        cp.wait()
    x = x_ref[...].astype(F32)
    inv = lax.rsqrt(jnp.mean(x * x, axis=-1, keepdims=True) + EPS)
    act_buf[...] = (x * inv * ga_ref[...].astype(F32).reshape(1, HIDDEN)).astype(BF16)
    normed = act_buf[...]
    sub = lax.broadcasted_iota(jnp.int32, (8, HEAD_DIM), 0)
    tiles = []
    for t in range(ROWS // 8):
        tile = jnp.zeros((8, HEAD_DIM), jnp.int32)
        for r in range(8):
            tile = jnp.where(sub == r, len_ref[t * 8 + r], tile)
        tiles.append(tile)
    angles = jnp.concatenate(tiles, axis=0).astype(F32) * freq_ref[...]
    lane = lax.broadcasted_iota(jnp.int32, (ROWS, HEAD_DIM), 1)
    even = (lane % 2) == 0
    turned = lane < HEAD_DIM // 2
    cosine = jnp.where(turned, jnp.cos(angles), 1.0)
    sine = jnp.sin(angles)
    sine = jnp.where(turned, jnp.where(even, -sine, sine), 0.0)
    bias = b_ref[...].astype(F32).reshape(1, HIDDEN + 2 * KV * HEAD_DIM)

    def rotate(v):
        swapped = jnp.where(even, pltpu.roll(v, HEAD_DIM - 1, 1), pltpu.roll(v, 1, 1))
        return v * cosine + swapped * sine

    for c in range(N_QKV):
        wq_copy(c).wait()
        fetch(c + WINDOW)
        acc = jnp.dot(normed, wq_buf[c], preferred_element_type=F32) + bias[:, c * QKV_CHUNK:(c + 1) * QKV_CHUNK]
        for t in range(QKV_CHUNK // HEAD_DIM):
            head = c * (QKV_CHUNK // HEAD_DIM) + t
            part = acc[:, t * HEAD_DIM:(t + 1) * HEAD_DIM]
            if head < HEADS:
                q_scr[pl.ds(head, ROWS, stride=HEADS), :] = rotate(part)
            elif head < HEADS + KV:
                kn_scr[head - HEADS] = rotate(part)
            else:
                vn_scr[head - HEADS - KV] = part

    row16 = lax.broadcasted_iota(jnp.int32, (16, HEAD_DIM), 0)
    col = lax.broadcasted_iota(jnp.int32, (HEADS, FLAT), 1)
    row32 = lax.broadcasted_iota(jnp.int32, (2 * HEADS, HEAD_DIM), 0)
    head_row = lax.broadcasted_iota(jnp.int32, (HEADS, FLAT), 0)
    pos = jnp.where((col % KV) == (head_row // (HEADS // KV)), col // KV, 2 * LMAX)

    def insert(i):
        for u in range(SEQ_CHUNK):
            b = i * SEQ_CHUNK + u
            ln = len_ref[b]
            base = pl.multiple_of((ln // 8) * 16, 16)
            hit = (row16 // 2) == (ln % 8)
            for buf, new in ((k_buf, kn_scr), (v_buf, vn_scr)):
                fresh = jnp.where(row16 % 2 == 0, new[0, pl.ds(b, 1), :], new[1, pl.ds(b, 1), :])
                old = buf[b, pl.ds(base, 16), :].astype(F32)
                buf[b, pl.ds(base, 16), :] = jnp.where(hit, fresh, old).astype(BF16)

    def scores(i):
        out = []
        for u in range(0, SEQ_CHUNK, 2):
            b = i * SEQ_CHUNK + u
            q = q_scr[pl.ds(b * HEADS, 2 * HEADS), :]
            first = row32 < HEADS
            q2 = jnp.concatenate([jnp.where(first, q, 0.0), jnp.where(first, 0.0, q)], axis=1).astype(BF16)
            k2 = jnp.concatenate([k_buf[b], k_buf[b + 1]], axis=1)
            out.append(lax.dot_general(q2, k2, (((1,), (1,)), ((), ())), preferred_element_type=F32))
        return out

    def probabilities(i, raw):
        probs = []
        for u in range(0, SEQ_CHUNK, 2):
            b = i * SEQ_CHUNK + u
            s2 = raw[u // 2]
            pair = []
            for t in range(2):
                s = jnp.where(pos <= len_ref[b + t], s2[t * HEADS:(t + 1) * HEADS], -jnp.inf)
                e = jnp.exp((s - jnp.max(s, axis=1, keepdims=True)) * (HEAD_DIM ** -0.5))
                pair.append((e * (1.0 / jnp.sum(e, axis=1, keepdims=True))).astype(BF16))
            probs.append(jnp.concatenate(pair, axis=0))
        return probs

    def weighted_values(i, probs):
        for u in range(0, SEQ_CHUNK, 2):
            b = i * SEQ_CHUNK + u
            v2 = jnp.concatenate([v_buf[b], v_buf[b + 1]], axis=1)
            c2 = jnp.dot(probs[u // 2], v2, preferred_element_type=F32)
            ctx_scr[pl.ds(b * HEADS, HEADS), :] = c2[:HEADS, :HEAD_DIM]
            ctx_scr[pl.ds((b + 1) * HEADS, HEADS), :] = c2[HEADS:, HEAD_DIM:]

    probs = None
    for i in range(N_SEQ):
        k_copy(i).wait()
        v_copy(i).wait()
        fetch(N_QKV + i + WINDOW)
        if i >= OUT_LAG:
            ko_copy(i - OUT_LAG).start()
            vo_copy(i - OUT_LAG).start()
        insert(i)
        raw = scores(i)
        if i > 0:
            weighted_values(i - 1, probs)
        probs = probabilities(i, raw)
    for i in range(N_SEQ - OUT_LAG, N_SEQ):
        ko_copy(i).start()
        vo_copy(i).start()
    weighted_values(N_SEQ - 1, probs)

    for h in range(HEADS):
        act_buf[:, h * HEAD_DIM:(h + 1) * HEAD_DIM] = ctx_scr[pl.ds(h, ROWS, stride=HEADS), :].astype(BF16)
    ctx = act_buf[...]
    total = jnp.zeros((ROWS, 1), F32)
    for c in range(N_PROJ):
        wp_copy(c).wait()
        cols = slice(c * PROJ_CHUNK, (c + 1) * PROJ_CHUNK)
        hid = x_ref[:, cols].astype(F32) + jnp.dot(ctx, wp_buf[c], preferred_element_type=F32)
        h_ref[:, cols] = hid
        total = total + jnp.sum(hid * hid, axis=-1, keepdims=True)
    inv2 = lax.rsqrt(total * (1.0 / HIDDEN) + EPS)
    m_ref[...] = (h_ref[...] * inv2 * gm_ref[...].astype(F32).reshape(1, HIDDEN)).astype(BF16)
    h_copy = pltpu.make_async_copy(h_ref, h_hbm.at[pl.ds(0, ROWS)], out_sem.at[0])
    m_copy = pltpu.make_async_copy(m_ref, m_hbm.at[pl.ds(0, ROWS)], out_sem.at[1])
    h_copy.start()
    m_copy.start()
    for i in range(N_SEQ):
        ko_copy(i).wait()
        vo_copy(i).wait()
    h_copy.wait()
    m_copy.wait()


def attention(lens, freq, x, ga, gm, bias, w_qkv, k_flat, v_flat, w_proj):
    hbm = pl.BlockSpec(memory_space=pl.ANY)
    smem = pl.BlockSpec(memory_space=pltpu.SMEM)
    dma = pltpu.SemaphoreType.DMA
    return pl.pallas_call(
        attn_kernel,
        out_shape=(jax.ShapeDtypeStruct((HBM_ROWS, HIDDEN), F32), jax.ShapeDtypeStruct((HBM_ROWS, HIDDEN), BF16),
                   jax.ShapeDtypeStruct(k_flat.shape, BF16), jax.ShapeDtypeStruct(v_flat.shape, BF16)),
        in_specs=[smem] + [hbm] * 9,
        out_specs=(hbm,) * 4,
        scratch_shapes=[
            pltpu.VMEM((1, HEAD_DIM), F32), pltpu.VMEM((ROWS, HIDDEN), BF16), pltpu.VMEM((HIDDEN,), BF16),
            pltpu.VMEM((HIDDEN,), BF16), pltpu.VMEM((HIDDEN + 2 * KV * HEAD_DIM,), BF16),
            pltpu.VMEM((ROWS, HIDDEN), F32), pltpu.VMEM((ROWS, HIDDEN), BF16),
            pltpu.VMEM((N_QKV, HIDDEN, QKV_CHUNK), BF16),
            pltpu.VMEM((N_PROJ, HIDDEN, PROJ_CHUNK), BF16),
            pltpu.VMEM((ROWS, FLAT, HEAD_DIM), BF16),
            pltpu.VMEM((ROWS, FLAT, HEAD_DIM), BF16),
            pltpu.VMEM((ROWS * HEADS, HEAD_DIM), F32),
            pltpu.VMEM((KV, ROWS, HEAD_DIM), F32),
            pltpu.VMEM((KV, ROWS, HEAD_DIM), F32),
            pltpu.VMEM((ROWS * HEADS, HEAD_DIM), F32),
            pltpu.VMEM((ROWS, HIDDEN), BF16),
            dma((5,)), dma((N_QKV,)), dma((N_PROJ,)), dma((N_SEQ,)), dma((N_SEQ,)), dma((2,)),
        ],
        compiler_params=pltpu.CompilerParams(vmem_limit_bytes=60 * 1024 * 1024),
        name="attn_block",
    )(lens, freq, x, ga, gm, bias, w_qkv, k_flat, v_flat, w_proj)


def mlp_kernel(m_hbm, h_hbm, win_hbm, wout_hbm, y_ref,
               m_ref, h_ref, rows_buf, part_acc, late_acc, win_buf, wint_buf, wout_buf, g_buf, pair_send, pair_recv, near_send, near_recv, far_keep, far_send, far_recv,
               own_acc, direct_send, direct_recv, in_sem, win_sem, wout_sem, agx_s, agx_r, agp_s, agp_r, agr_s, agr_r,
               ps_s, ps_r, ns_s, ns_r, fs_s, fs_r, ds_s, ds_r):
    me = lax.axis_index('grp')
    partner = me + 1 - 2 * (me % 2)
    cross = (me + 2) % 4
    diag = (partner + 2) % 4

    def win_copy(i, width):
        src = win_hbm.at[:, pl.ds(i * F_CHUNK, width)]
        return pltpu.make_async_copy(src, win_buf.at[i % RING, :, pl.ds(0, width)], win_sem.at[i % RING])

    def wout_copy(j):
        rows = pl.ds(j * W_ROWS, W_ROWS)
        return pltpu.make_async_copy(wout_hbm.at[rows], wout_buf.at[rows], wout_sem.at[j])

    m_copy = pltpu.make_async_copy(m_hbm.at[pl.ds(0, ROWS)], m_ref, in_sem.at[0])
    h_copy = pltpu.make_async_copy(h_hbm.at[pl.ds(0, ROWS)], h_ref, in_sem.at[1])
    m_copy.start()
    tail = FFN_LOC - (N_F - 1) * F_CHUNK
    widths = [F_CHUNK] * (N_F - 1) + [tail]
    first_copies = [pltpu.make_async_copy(win_hbm.at[part, pl.ds(0, F_CHUNK)], win_buf.at[0, part],
                                          win_sem.at[part * RING]) for part in range(2)]
    for cp in first_copies:
        cp.start(priority=1)
    for i in range(1, RING):
        win_copy(i, widths[i]).start(priority=1)
    h_copy.start()

    barrier = pltpu.get_barrier_semaphore()
    for peer in (partner, cross, diag):
        pl.semaphore_signal(barrier, inc=1, device_id={'grp': peer}, device_id_type=pl.DeviceIdType.MESH)
    pl.semaphore_wait(barrier, 3)

    def send(src, dst, ssem, rsem, peer):
        return pltpu.make_async_remote_copy(src_ref=src, dst_ref=dst, send_sem=ssem, recv_sem=rsem,
                                            device_id={'grp': peer}, device_id_type=pl.DeviceIdType.MESH)

    def part_of(slot, p):
        return rows_buf.at[pl.ds(slot * ROWS, ROWS), pl.ds(p * AG_COLS, AG_COLS)]

    cross_copies = [send(m_ref.at[:, pl.ds(p * AG_COLS, AG_COLS)], part_of(2, p), agx_s.at[p], agx_r.at[p], cross)
                    for p in range(AG_PIECES)]
    m_copy.wait()
    for cp in cross_copies:
        cp.start()
    pair_copy = send(m_ref, rows_buf.at[pl.ds(ROWS, ROWS)], agp_s, agp_r, partner)
    pair_copy.start()
    rows_buf[pl.ds(0, ROWS), :] = m_ref[...]
    relays = [send(part_of(2, p), part_of(3, p), agr_s.at[p], agr_r.at[p], partner) for p in range(AG_PIECES)]

    def gated(gate, up):
        return (gate * jax.nn.sigmoid(gate) * up).astype(BF16)

    def local_ffn(i):
        rows = rows_buf[pl.ds(0, 2 * ROWS), :]
        gate, up = [jnp.dot(rows, wint_buf[i, part, :, :widths[i]], preferred_element_type=F32) for part in range(2)]
        g_buf[pl.ds(0, 2 * ROWS), pl.ds(i * F_CHUNK, widths[i])] = gated(gate, up)

    def ahead_chunk(i, phase):
        k0, size = K_PARTS[phase]
        rows = rows_buf[pl.ds(2 * ROWS, 2 * ROWS), k0:k0 + size]
        cols = pl.ds(i * F_CHUNK, widths[i])
        sums = []
        for part in range(2):
            prod = jnp.dot(rows, wint_buf[i, part, k0:k0 + size, :], preferred_element_type=F32)
            sums.append(prod if phase == 0 else part_acc[part, :, cols] + prod)
        if phase < len(K_PARTS) - 1:
            for part in range(2):
                part_acc[part, :, cols] = sums[part]
        else:
            g_buf[pl.ds(2 * ROWS, 2 * ROWS), cols] = gated(sums[0], sums[1])

    def late_chunk(i, phase):
        k0, size = K_PARTS[phase]
        rows = rows_buf[:, k0:k0 + size]
        cols = pl.ds((i - N_T) * F_CHUNK, widths[i])
        sums = []
        for part in range(2):
            prod = lax.dot_general(rows, win_buf[i % RING, part, :widths[i], k0:k0 + size],
                                   (((1,), (1,)), ((), ())), preferred_element_type=F32)
            sums.append(prod if phase == 0 else late_acc[part, :, cols] + prod)
        if phase < len(K_PARTS) - 1:
            for part in range(2):
                late_acc[part, :, cols] = sums[part]
        else:
            g_buf[:, pl.ds(i * F_CHUNK, widths[i])] = gated(sums[0], sums[1])

    def remote_phase(phase, first, last):
        for i in range(first, last):
            (ahead_chunk if i < N_T else late_chunk)(i, phase)

    def relay(p):
        cross_copies[p].wait_recv()
        relays[p].start()

    for i in range(N_T):
        if i == 1:
            pair_copy.wait()
        if i > 0:
            win_copy(i, widths[i]).wait()
        for part in range(2):
            if i == 0:
                first_copies[part].wait()
            wint_buf[i, part] = win_buf[i % RING, part].T
        if i + RING < N_F:
            win_copy(i + RING, widths[i + RING]).start(priority=1)
        else:
            wout_copy(i + RING - N_F).start(priority=1)
        if i >= 1:
            local_ffn(i - 1)
        if i in RELAY_AT:
            relay(RELAY_AT.index(i))
    for j in range(N_T + RING - N_F, N_W):
        wout_copy(j).start(priority=1)
    local_ffn(N_T - 1)
    for i in range(N_T, N_F):
        win_copy(i, widths[i]).wait()
    if len(RELAY_AT) < 3:
        relay(2)
    for p in range(2):
        relays[p].wait_recv()
    remote_phase(0, 0, CUT)
    relay(3)
    remote_phase(0, CUT, N_F)
    relays[2].wait_recv()
    relays[3].wait_recv()
    remote_phase(1, 0, N_F)
    for p in range(AG_PIECES):
        cross_copies[p].wait_send()
        relays[p].wait_send()
    for j in range(N_W):
        wout_copy(j).wait()
    h_copy.wait()

    def piece(k, shared=False):
        start = max(D_EDGES[k], DIRECT) if shared else D_EDGES[k]
        return pl.ds(start, D_EDGES[k + 1] - start)

    def block_send(src, dst, ssem, rsem, peer, shared=True):
        return [send(src.at[:, piece(k, shared)], dst.at[:, piece(k, shared)], ssem.at[k], rsem.at[k], peer) for k in range(N_D)]

    pair_copies = block_send(pair_send, pair_recv, ps_s, ps_r, partner)
    near_copies = block_send(near_send, near_recv, ns_s, ns_r, partner, shared=False)
    far_copies = block_send(far_send, far_recv, fs_s, fs_r, cross)

    direct_copies = [send(direct_send.at[pl.ds(n * ROWS, ROWS)], direct_recv.at[pl.ds(n * ROWS, ROWS)],
                          ds_s.at[n], ds_r.at[n], (cross, diag)[n]) for n in range(2)]

    def down(rows, k):
        return jnp.dot(g_buf[rows, :], wout_buf[:, piece(k)], preferred_element_type=F32)

    def remote_block(k):
        part = down(slice(2 * ROWS, 4 * ROWS), k)
        if k == 0:
            direct_send[...] = part[:, :DIRECT].astype(BF16)
            for cp in direct_copies:
                cp.start()
            part = part[:, DIRECT:]
        far_keep[:, piece(k, True)] = part[:ROWS]
        pair_send[:, piece(k, True)] = part[ROWS:].astype(BF16)
        pair_copies[k].start()

    def local_block(k):
        part = down(slice(0, 2 * ROWS), k)
        own_acc[:, piece(k)] = part[:ROWS] + h_ref[:, piece(k)]
        near_send[:, piece(k)] = part[ROWS:].astype(BF16)
        near_copies[k].start()

    def pair_sum(k):
        cols = piece(k, True)
        pair_copies[k].wait_recv()
        far_send[:, cols] = (far_keep[:, cols] + pair_recv[:, cols].astype(F32)).astype(BF16)
        far_copies[k].start()

    steps = [(remote_block, k) for k in range(N_D)] + [(local_block, k) for k in range(N_D)]
    for n, (step, k) in enumerate(steps):
        step(k)
        if 0 <= n - PAIR_LAG < N_D:
            pair_sum(n - PAIR_LAG)
    for cp in direct_copies:
        cp.wait()
    for k in range(N_D):
        near_copies[k].wait_recv()
        near = own_acc[:, piece(k)] + near_recv[:, piece(k)].astype(F32)
        if k == 0:
            direct = direct_recv[...].astype(F32)
            y_ref[:, :DIRECT] = (near[:, :DIRECT] + direct[:ROWS] + direct[ROWS:]).astype(BF16)
            near = near[:, DIRECT:]
        far_copies[k].wait_recv()
        y_ref[:, piece(k, True)] = (near + far_recv[:, piece(k, True)].astype(F32)).astype(BF16)
    for k in range(N_D):
        pair_copies[k].wait_send()
        near_copies[k].wait_send()
        far_copies[k].wait_send()


def mlp(m, h, w_in, w_out):
    vmem = pl.BlockSpec(memory_space=pltpu.VMEM)
    hbm = pl.BlockSpec(memory_space=pl.ANY)
    dma = pltpu.SemaphoreType.DMA
    piece = (ROWS, HIDDEN)
    return pl.pallas_call(
        mlp_kernel,
        out_shape=jax.ShapeDtypeStruct((ROWS, HIDDEN), BF16),
        in_specs=[hbm] * 4,
        out_specs=vmem,
        scratch_shapes=[
            pltpu.VMEM((ROWS, HIDDEN), BF16), pltpu.VMEM((ROWS, HIDDEN), F32),
            pltpu.VMEM((4 * ROWS, HIDDEN), BF16),
            pltpu.VMEM((2, 2 * ROWS, N_T * F_CHUNK), F32),
            pltpu.VMEM((2, 4 * ROWS, (N_F - N_T) * F_CHUNK), F32),
            pltpu.VMEM((RING, 2, F_CHUNK, HIDDEN), BF16),
            pltpu.VMEM((N_T, 2, HIDDEN, F_CHUNK), BF16),
            pltpu.VMEM((FFN_LOC, HIDDEN), BF16),
            pltpu.VMEM((4 * ROWS, FFN_LOC), BF16),
            pltpu.VMEM(piece, BF16), pltpu.VMEM(piece, BF16),
            pltpu.VMEM(piece, BF16), pltpu.VMEM(piece, BF16),
            pltpu.VMEM(piece, F32), pltpu.VMEM(piece, BF16), pltpu.VMEM(piece, BF16),
            pltpu.VMEM(piece, F32),
            pltpu.VMEM((2 * ROWS, DIRECT), BF16), pltpu.VMEM((2 * ROWS, DIRECT), BF16),
            dma((2,)), dma((RING + 1,)), dma((N_W,)),
            dma((AG_PIECES,)), dma((AG_PIECES,)), dma, dma, dma((AG_PIECES,)), dma((AG_PIECES,)),
            dma((N_D,)), dma((N_D,)), dma((N_D,)), dma((N_D,)), dma((N_D,)), dma((N_D,)), dma((2,)), dma((2,)),
        ],
        compiler_params=pltpu.CompilerParams(vmem_limit_bytes=50 * 1024 * 1024, collective_id=0, has_side_effects=True),
        name="mlp_block",
    )(m, h, w_in, w_out)


def rope_freq():
    pair = 2 * (np.arange(HEAD_DIM) // 2)
    return jnp.asarray((ROPE_BASE ** (-pair / (HEAD_DIM // 2)))[None, :], F32)


def solution(mesh):
    row_spec = P(('rep', 'grp'))
    repl_spec = P()

    def local_layer(x_in, seq_len, k_cache, v_cache, gamma_attn, w_qkv, b_qkv, w_proj, gamma_mlp, w_in, w_out):
        k_flat = k_cache.reshape(ROWS, FLAT, HEAD_DIM)
        v_flat = v_cache.reshape(ROWS, FLAT, HEAD_DIM)
        h, m, k_out, v_out = attention(seq_len, rope_freq(), x_in, gamma_attn, gamma_mlp, b_qkv, w_qkv, k_flat, v_flat, w_proj)
        layer_out = mlp(m, h, w_in, w_out)
        return layer_out, k_out.reshape(k_cache.shape), v_out.reshape(v_cache.shape)

    return jax.shard_map(local_layer, mesh=mesh,
                         in_specs=(row_spec, row_spec, row_spec, row_spec, repl_spec, repl_spec, repl_spec,
                                   repl_spec, repl_spec, P(None, 'grp', None), P('grp', None)),
                         out_specs=(row_spec, row_spec, row_spec), check_vma=False)
```

```python
import jax
import jax.numpy as jnp
import numpy as np
from jax import lax
from jax.experimental import pallas as pl
from jax.experimental.pallas import tpu as pltpu
from jax.sharding import PartitionSpec as P

HEAD_DIM = 128
ROPE_BASE = 10000.0
EPS = 1e-5
HIDDEN = 2048
HEADS = 16
KV = 2
ROWS = 64
LMAX = 256
FLAT = LMAX * KV
FFN_LOC = 2752
QKV_CHUNK = 512
N_QKV = 5
PROJ_CHUNK = 512
N_PROJ = 4
SEQ_CHUNK = 8
N_SEQ = ROWS // SEQ_CHUNK
WINDOW = 7
OUT_LAG = 4
F_CHUNK = 256
N_F = 11
DIRECT = 256
D_EDGES = (0, 512, 1024, 1536, 2048)
N_D = len(D_EDGES) - 1
PAIR_LAG = 2
AG_PIECES = 4
AG_COLS = HIDDEN // AG_PIECES
K_PARTS = ((0, HIDDEN // 2), (HIDDEN // 2, HIDDEN // 2))
RING = 4
CUT = 4
N_T = 9
N_W = 4
W_ROWS = FFN_LOC // N_W
RELAY_AT = (4, 6)
HBM_ROWS = 2048
F32 = jnp.float32
BF16 = jnp.bfloat16


def attn_kernel(len_ref, freq_hbm, x_hbm, ga_hbm, gm_hbm, b_hbm, wqkv_hbm, k_hbm, v_hbm, wproj_hbm,
                h_hbm, m_hbm, kout_hbm, vout_hbm,
                freq_ref, x_ref, ga_ref, gm_ref, b_ref, h_ref, m_ref,
                wq_buf, wp_buf, k_buf, v_buf, q_scr, kn_scr, vn_scr, ctx_scr, act_buf,
                small_sem, wq_sem, wp_sem, k_sem, v_sem, out_sem):
    small = [pltpu.make_async_copy(src, dst, small_sem.at[n]) for n, (src, dst) in enumerate(
        ((x_hbm, x_ref), (ga_hbm, ga_ref), (freq_hbm, freq_ref), (b_hbm, b_ref), (gm_hbm, gm_ref)))]

    def wq_copy(c):
        return pltpu.make_async_copy(wqkv_hbm.at[:, pl.ds(c * QKV_CHUNK, QKV_CHUNK)], wq_buf.at[c], wq_sem.at[c])

    def wp_copy(c):
        return pltpu.make_async_copy(wproj_hbm.at[:, pl.ds(c * PROJ_CHUNK, PROJ_CHUNK)], wp_buf.at[c], wp_sem.at[c])

    def k_copy(i):
        rows = pl.ds(i * SEQ_CHUNK, SEQ_CHUNK)
        return pltpu.make_async_copy(k_hbm.at[rows], k_buf.at[rows], k_sem.at[i])

    def v_copy(i):
        rows = pl.ds(i * SEQ_CHUNK, SEQ_CHUNK)
        return pltpu.make_async_copy(v_hbm.at[rows], v_buf.at[rows], v_sem.at[i])

    def ko_copy(i):
        rows = pl.ds(i * SEQ_CHUNK, SEQ_CHUNK)
        return pltpu.make_async_copy(k_buf.at[rows], kout_hbm.at[rows], k_sem.at[i])

    def vo_copy(i):
        rows = pl.ds(i * SEQ_CHUNK, SEQ_CHUNK)
        return pltpu.make_async_copy(v_buf.at[rows], vout_hbm.at[rows], v_sem.at[i])

    for cp in small:
        cp.start()
    def fetch(n):
        if n < N_QKV:
            wq_copy(n).start()
        elif n < N_QKV + N_SEQ:
            k_copy(n - N_QKV).start()
            v_copy(n - N_QKV).start()
        elif n < N_QKV + N_SEQ + N_PROJ:
            wp_copy(n - N_QKV - N_SEQ).start()

    for n in range(WINDOW):
        fetch(n)

    for cp in small:
        cp.wait()
    x = x_ref[...].astype(F32)
    inv = lax.rsqrt(jnp.mean(x * x, axis=-1, keepdims=True) + EPS)
    act_buf[...] = (x * inv * ga_ref[...].astype(F32).reshape(1, HIDDEN)).astype(BF16)
    normed = act_buf[...]
    sub = lax.broadcasted_iota(jnp.int32, (8, HEAD_DIM), 0)
    tiles = []
    for t in range(ROWS // 8):
        tile = jnp.zeros((8, HEAD_DIM), jnp.int32)
        for r in range(8):
            tile = jnp.where(sub == r, len_ref[t * 8 + r], tile)
        tiles.append(tile)
    angles = jnp.concatenate(tiles, axis=0).astype(F32) * freq_ref[...]
    lane = lax.broadcasted_iota(jnp.int32, (ROWS, HEAD_DIM), 1)
    even = (lane % 2) == 0
    turned = lane < HEAD_DIM // 2
    cosine = jnp.where(turned, jnp.cos(angles), 1.0)
    sine = jnp.sin(angles)
    sine = jnp.where(turned, jnp.where(even, -sine, sine), 0.0)
    bias = b_ref[...].astype(F32).reshape(1, HIDDEN + 2 * KV * HEAD_DIM)

    def rotate(v):
        swapped = jnp.where(even, pltpu.roll(v, HEAD_DIM - 1, 1), pltpu.roll(v, 1, 1))
        return v * cosine + swapped * sine

    for c in range(N_QKV):
        wq_copy(c).wait()
        fetch(c + WINDOW)
        acc = jnp.dot(normed, wq_buf[c], preferred_element_type=F32) + bias[:, c * QKV_CHUNK:(c + 1) * QKV_CHUNK]
        for t in range(QKV_CHUNK // HEAD_DIM):
            head = c * (QKV_CHUNK // HEAD_DIM) + t
            part = acc[:, t * HEAD_DIM:(t + 1) * HEAD_DIM]
            if head < HEADS:
                q_scr[pl.ds(head, ROWS, stride=HEADS), :] = rotate(part)
            elif head < HEADS + KV:
                kn_scr[head - HEADS] = rotate(part)
            else:
                vn_scr[head - HEADS - KV] = part

    row16 = lax.broadcasted_iota(jnp.int32, (16, HEAD_DIM), 0)
    col = lax.broadcasted_iota(jnp.int32, (HEADS, FLAT), 1)
    row32 = lax.broadcasted_iota(jnp.int32, (2 * HEADS, HEAD_DIM), 0)
    head_row = lax.broadcasted_iota(jnp.int32, (HEADS, FLAT), 0)
    pos = jnp.where((col % KV) == (head_row // (HEADS // KV)), col // KV, 2 * LMAX)

    def insert(i):
        for u in range(SEQ_CHUNK):
            b = i * SEQ_CHUNK + u
            ln = len_ref[b]
            base = pl.multiple_of((ln // 8) * 16, 16)
            hit = (row16 // 2) == (ln % 8)
            for buf, new in ((k_buf, kn_scr), (v_buf, vn_scr)):
                fresh = jnp.where(row16 % 2 == 0, new[0, pl.ds(b, 1), :], new[1, pl.ds(b, 1), :])
                old = buf[b, pl.ds(base, 16), :].astype(F32)
                buf[b, pl.ds(base, 16), :] = jnp.where(hit, fresh, old).astype(BF16)

    def scores(i):
        out = []
        for u in range(0, SEQ_CHUNK, 2):
            b = i * SEQ_CHUNK + u
            q = q_scr[pl.ds(b * HEADS, 2 * HEADS), :]
            first = row32 < HEADS
            q2 = jnp.concatenate([jnp.where(first, q, 0.0), jnp.where(first, 0.0, q)], axis=1).astype(BF16)
            k2 = jnp.concatenate([k_buf[b], k_buf[b + 1]], axis=1)
            out.append(lax.dot_general(q2, k2, (((1,), (1,)), ((), ())), preferred_element_type=F32))
        return out

    def probabilities(i, raw):
        probs = []
        for u in range(0, SEQ_CHUNK, 2):
            b = i * SEQ_CHUNK + u
            s2 = raw[u // 2]
            pair = []
            for t in range(2):
                s = jnp.where(pos <= len_ref[b + t], s2[t * HEADS:(t + 1) * HEADS], -jnp.inf)
                e = jnp.exp((s - jnp.max(s, axis=1, keepdims=True)) * (HEAD_DIM ** -0.5))
                pair.append((e * (1.0 / jnp.sum(e, axis=1, keepdims=True))).astype(BF16))
            probs.append(jnp.concatenate(pair, axis=0))
        return probs

    def weighted_values(i, probs):
        for u in range(0, SEQ_CHUNK, 2):
            b = i * SEQ_CHUNK + u
            v2 = jnp.concatenate([v_buf[b], v_buf[b + 1]], axis=1)
            c2 = jnp.dot(probs[u // 2], v2, preferred_element_type=F32)
            ctx_scr[pl.ds(b * HEADS, HEADS), :] = c2[:HEADS, :HEAD_DIM]
            ctx_scr[pl.ds((b + 1) * HEADS, HEADS), :] = c2[HEADS:, HEAD_DIM:]

    probs = None
    for i in range(N_SEQ):
        k_copy(i).wait()
        v_copy(i).wait()
        fetch(N_QKV + i + WINDOW)
        if i >= OUT_LAG:
            ready = [i - OUT_LAG] if i < N_SEQ - 1 else range(i - OUT_LAG, N_SEQ - 1)
            for j in ready:
                ko_copy(j).start()
                vo_copy(j).start()
        insert(i)
        raw = scores(i)
        if i > 0:
            weighted_values(i - 1, probs)
        probs = probabilities(i, raw)
    ko_copy(N_SEQ - 1).start()
    vo_copy(N_SEQ - 1).start()
    weighted_values(N_SEQ - 1, probs)

    for h in range(HEADS):
        act_buf[:, h * HEAD_DIM:(h + 1) * HEAD_DIM] = ctx_scr[pl.ds(h, ROWS, stride=HEADS), :].astype(BF16)
    ctx = act_buf[...]
    total = jnp.zeros((ROWS, 1), F32)
    for c in range(N_PROJ):
        wp_copy(c).wait()
        cols = slice(c * PROJ_CHUNK, (c + 1) * PROJ_CHUNK)
        hid = x_ref[:, cols].astype(F32) + jnp.dot(ctx, wp_buf[c], preferred_element_type=F32)
        h_ref[:, cols] = hid
        total = total + jnp.sum(hid * hid, axis=-1, keepdims=True)
    inv2 = lax.rsqrt(total * (1.0 / HIDDEN) + EPS)
    m_ref[...] = (h_ref[...] * inv2 * gm_ref[...].astype(F32).reshape(1, HIDDEN)).astype(BF16)
    h_copy = pltpu.make_async_copy(h_ref, h_hbm.at[pl.ds(0, ROWS)], out_sem.at[0])
    m_copy = pltpu.make_async_copy(m_ref, m_hbm.at[pl.ds(0, ROWS)], out_sem.at[1])
    h_copy.start()
    m_copy.start()
    for i in range(N_SEQ):
        ko_copy(i).wait()
        vo_copy(i).wait()
    h_copy.wait()
    m_copy.wait()


def attention(lens, freq, x, ga, gm, bias, w_qkv, k_flat, v_flat, w_proj):
    hbm = pl.BlockSpec(memory_space=pl.ANY)
    smem = pl.BlockSpec(memory_space=pltpu.SMEM)
    dma = pltpu.SemaphoreType.DMA
    return pl.pallas_call(
        attn_kernel,
        out_shape=(jax.ShapeDtypeStruct((HBM_ROWS, HIDDEN), F32), jax.ShapeDtypeStruct((HBM_ROWS, HIDDEN), BF16),
                   jax.ShapeDtypeStruct(k_flat.shape, BF16), jax.ShapeDtypeStruct(v_flat.shape, BF16)),
        in_specs=[smem] + [hbm] * 9,
        out_specs=(hbm,) * 4,
        scratch_shapes=[
            pltpu.VMEM((1, HEAD_DIM), F32), pltpu.VMEM((ROWS, HIDDEN), BF16), pltpu.VMEM((HIDDEN,), BF16),
            pltpu.VMEM((HIDDEN,), BF16), pltpu.VMEM((HIDDEN + 2 * KV * HEAD_DIM,), BF16),
            pltpu.VMEM((ROWS, HIDDEN), F32), pltpu.VMEM((ROWS, HIDDEN), BF16),
            pltpu.VMEM((N_QKV, HIDDEN, QKV_CHUNK), BF16),
            pltpu.VMEM((N_PROJ, HIDDEN, PROJ_CHUNK), BF16),
            pltpu.VMEM((ROWS, FLAT, HEAD_DIM), BF16),
            pltpu.VMEM((ROWS, FLAT, HEAD_DIM), BF16),
            pltpu.VMEM((ROWS * HEADS, HEAD_DIM), F32),
            pltpu.VMEM((KV, ROWS, HEAD_DIM), F32),
            pltpu.VMEM((KV, ROWS, HEAD_DIM), F32),
            pltpu.VMEM((ROWS * HEADS, HEAD_DIM), F32),
            pltpu.VMEM((ROWS, HIDDEN), BF16),
            dma((5,)), dma((N_QKV,)), dma((N_PROJ,)), dma((N_SEQ,)), dma((N_SEQ,)), dma((2,)),
        ],
        compiler_params=pltpu.CompilerParams(vmem_limit_bytes=60 * 1024 * 1024),
        name="attn_block",
    )(lens, freq, x, ga, gm, bias, w_qkv, k_flat, v_flat, w_proj)


def mlp_kernel(m_hbm, h_hbm, win_hbm, wout_hbm, y_ref,
               m_ref, h_ref, rows_buf, part_acc, late_acc, win_buf, wint_buf, wout_buf, g_buf, pair_send, pair_recv, near_send, near_recv, far_keep, far_send, far_recv,
               own_acc, direct_send, direct_recv, in_sem, win_sem, wout_sem, agx_s, agx_r, agp_s, agp_r, agr_s, agr_r,
               ps_s, ps_r, ns_s, ns_r, fs_s, fs_r, ds_s, ds_r):
    me = lax.axis_index('grp')
    partner = me + 1 - 2 * (me % 2)
    cross = (me + 2) % 4
    diag = (partner + 2) % 4

    def win_copy(i, width):
        src = win_hbm.at[:, pl.ds(i * F_CHUNK, width)]
        return pltpu.make_async_copy(src, win_buf.at[i % RING, :, pl.ds(0, width)], win_sem.at[i % RING])

    def wout_copy(j):
        rows = pl.ds(j * W_ROWS, W_ROWS)
        return pltpu.make_async_copy(wout_hbm.at[rows], wout_buf.at[rows], wout_sem.at[j])

    m_copy = pltpu.make_async_copy(m_hbm.at[pl.ds(0, ROWS)], m_ref, in_sem.at[0])
    h_copy = pltpu.make_async_copy(h_hbm.at[pl.ds(0, ROWS)], h_ref, in_sem.at[1])
    m_copy.start()
    tail = FFN_LOC - (N_F - 1) * F_CHUNK
    widths = [F_CHUNK] * (N_F - 1) + [tail]
    first_copies = [pltpu.make_async_copy(win_hbm.at[part, pl.ds(0, F_CHUNK)], win_buf.at[0, part],
                                          win_sem.at[part * RING]) for part in range(2)]
    for cp in first_copies:
        cp.start(priority=1)
    for i in range(1, RING):
        win_copy(i, widths[i]).start(priority=1)
    h_copy.start()

    barrier = pltpu.get_barrier_semaphore()
    for peer in (partner, cross, diag):
        pl.semaphore_signal(barrier, inc=1, device_id={'grp': peer}, device_id_type=pl.DeviceIdType.MESH)
    pl.semaphore_wait(barrier, 3)

    def send(src, dst, ssem, rsem, peer):
        return pltpu.make_async_remote_copy(src_ref=src, dst_ref=dst, send_sem=ssem, recv_sem=rsem,
                                            device_id={'grp': peer}, device_id_type=pl.DeviceIdType.MESH)

    def part_of(slot, p):
        return rows_buf.at[pl.ds(slot * ROWS, ROWS), pl.ds(p * AG_COLS, AG_COLS)]

    cross_copies = [send(m_ref.at[:, pl.ds(p * AG_COLS, AG_COLS)], part_of(2, p), agx_s.at[p], agx_r.at[p], cross)
                    for p in range(AG_PIECES)]
    m_copy.wait()
    for cp in cross_copies:
        cp.start()
    pair_copy = send(m_ref, rows_buf.at[pl.ds(ROWS, ROWS)], agp_s, agp_r, partner)
    pair_copy.start()
    rows_buf[pl.ds(0, ROWS), :] = m_ref[...]
    relays = [send(part_of(2, p), part_of(3, p), agr_s.at[p], agr_r.at[p], partner) for p in range(AG_PIECES)]

    def gated(gate, up):
        return (gate * jax.nn.sigmoid(gate) * up).astype(BF16)

    def local_ffn(i):
        rows = rows_buf[pl.ds(0, 2 * ROWS), :]
        gate, up = [jnp.dot(rows, wint_buf[i, part, :, :widths[i]], preferred_element_type=F32) for part in range(2)]
        g_buf[pl.ds(0, 2 * ROWS), pl.ds(i * F_CHUNK, widths[i])] = gated(gate, up)

    def ahead_chunk(i, phase):
        k0, size = K_PARTS[phase]
        rows = rows_buf[pl.ds(2 * ROWS, 2 * ROWS), k0:k0 + size]
        cols = pl.ds(i * F_CHUNK, widths[i])
        sums = []
        for part in range(2):
            prod = jnp.dot(rows, wint_buf[i, part, k0:k0 + size, :], preferred_element_type=F32)
            sums.append(prod if phase == 0 else part_acc[part, :, cols] + prod)
        if phase < len(K_PARTS) - 1:
            for part in range(2):
                part_acc[part, :, cols] = sums[part]
        else:
            g_buf[pl.ds(2 * ROWS, 2 * ROWS), cols] = gated(sums[0], sums[1])

    def late_chunk(i, phase):
        k0, size = K_PARTS[phase]
        rows = rows_buf[:, k0:k0 + size]
        cols = pl.ds((i - N_T) * F_CHUNK, widths[i])
        sums = []
        for part in range(2):
            prod = lax.dot_general(rows, win_buf[i % RING, part, :widths[i], k0:k0 + size],
                                   (((1,), (1,)), ((), ())), preferred_element_type=F32)
            sums.append(prod if phase == 0 else late_acc[part, :, cols] + prod)
        if phase < len(K_PARTS) - 1:
            for part in range(2):
                late_acc[part, :, cols] = sums[part]
        else:
            g_buf[:, pl.ds(i * F_CHUNK, widths[i])] = gated(sums[0], sums[1])

    def remote_phase(phase, first, last):
        for i in range(first, last):
            (ahead_chunk if i < N_T else late_chunk)(i, phase)

    def relay(p):
        cross_copies[p].wait_recv()
        relays[p].start()

    for i in range(N_T):
        if i == 1:
            pair_copy.wait()
        if i > 0:
            win_copy(i, widths[i]).wait()
        for part in range(2):
            if i == 0:
                first_copies[part].wait()
            wint_buf[i, part] = win_buf[i % RING, part].T
        if i + RING < N_F:
            win_copy(i + RING, widths[i + RING]).start(priority=1)
        else:
            wout_copy(i + RING - N_F).start(priority=1)
        if i >= 1:
            local_ffn(i - 1)
        if i in RELAY_AT:
            relay(RELAY_AT.index(i))
    for j in range(N_T + RING - N_F, N_W):
        wout_copy(j).start(priority=1)
    local_ffn(N_T - 1)
    if len(RELAY_AT) < 3:
        relay(2)
    for i in range(N_T, N_F):
        win_copy(i, widths[i]).wait()
    for p in range(2):
        relays[p].wait_recv()
    remote_phase(0, 0, CUT)
    relay(3)
    remote_phase(0, CUT, N_F)
    relays[2].wait_recv()
    relays[3].wait_recv()
    remote_phase(1, 0, N_F)
    for p in range(AG_PIECES):
        cross_copies[p].wait_send()
        relays[p].wait_send()
    for j in range(N_W):
        wout_copy(j).wait()
    h_copy.wait()

    def piece(k, shared=False):
        start = max(D_EDGES[k], DIRECT) if shared else D_EDGES[k]
        return pl.ds(start, D_EDGES[k + 1] - start)

    def block_send(src, dst, ssem, rsem, peer, shared=True):
        return [send(src.at[:, piece(k, shared)], dst.at[:, piece(k, shared)], ssem.at[k], rsem.at[k], peer) for k in range(N_D)]

    pair_copies = block_send(pair_send, pair_recv, ps_s, ps_r, partner)
    near_copies = block_send(near_send, near_recv, ns_s, ns_r, partner, shared=False)
    far_copies = block_send(far_send, far_recv, fs_s, fs_r, cross)

    direct_copies = [send(direct_send.at[pl.ds(n * ROWS, ROWS)], direct_recv.at[pl.ds(n * ROWS, ROWS)],
                          ds_s.at[n], ds_r.at[n], (cross, diag)[n]) for n in range(2)]

    def down(rows, k):
        return jnp.dot(g_buf[rows, :], wout_buf[:, piece(k)], preferred_element_type=F32)

    def remote_block(k):
        part = down(slice(2 * ROWS, 4 * ROWS), k)
        if k == 0:
            direct_send[...] = part[:, :DIRECT].astype(BF16)
            for cp in direct_copies:
                cp.start()
            part = part[:, DIRECT:]
        far_keep[:, piece(k, True)] = part[:ROWS]
        pair_send[:, piece(k, True)] = part[ROWS:].astype(BF16)
        pair_copies[k].start()

    def local_block(k):
        part = down(slice(0, 2 * ROWS), k)
        own_acc[:, piece(k)] = part[:ROWS] + h_ref[:, piece(k)]
        near_send[:, piece(k)] = part[ROWS:].astype(BF16)
        near_copies[k].start()

    def pair_sum(k):
        cols = piece(k, True)
        pair_copies[k].wait_recv()
        far_send[:, cols] = (far_keep[:, cols] + pair_recv[:, cols].astype(F32)).astype(BF16)
        far_copies[k].start()

    steps = [(remote_block, k) for k in range(N_D)] + [(local_block, k) for k in range(N_D)]
    for n, (step, k) in enumerate(steps):
        step(k)
        if 0 <= n - PAIR_LAG < N_D:
            pair_sum(n - PAIR_LAG)
    for cp in direct_copies:
        cp.wait()
    for k in range(N_D):
        near_copies[k].wait_recv()
        near = own_acc[:, piece(k)] + near_recv[:, piece(k)].astype(F32)
        if k == 0:
            direct = direct_recv[...].astype(F32)
            y_ref[:, :DIRECT] = (near[:, :DIRECT] + direct[:ROWS] + direct[ROWS:]).astype(BF16)
            near = near[:, DIRECT:]
        far_copies[k].wait_recv()
        y_ref[:, piece(k, True)] = (near + far_recv[:, piece(k, True)].astype(F32)).astype(BF16)
    for k in range(N_D):
        pair_copies[k].wait_send()
        near_copies[k].wait_send()
        far_copies[k].wait_send()


def mlp(m, h, w_in, w_out):
    vmem = pl.BlockSpec(memory_space=pltpu.VMEM)
    hbm = pl.BlockSpec(memory_space=pl.ANY)
    dma = pltpu.SemaphoreType.DMA
    piece = (ROWS, HIDDEN)
    return pl.pallas_call(
        mlp_kernel,
        out_shape=jax.ShapeDtypeStruct((ROWS, HIDDEN), BF16),
        in_specs=[hbm] * 4,
        out_specs=vmem,
        scratch_shapes=[
            pltpu.VMEM((ROWS, HIDDEN), BF16), pltpu.VMEM((ROWS, HIDDEN), F32),
            pltpu.VMEM((4 * ROWS, HIDDEN), BF16),
            pltpu.VMEM((2, 2 * ROWS, N_T * F_CHUNK), F32),
            pltpu.VMEM((2, 4 * ROWS, (N_F - N_T) * F_CHUNK), F32),
            pltpu.VMEM((RING, 2, F_CHUNK, HIDDEN), BF16),
            pltpu.VMEM((N_T, 2, HIDDEN, F_CHUNK), BF16),
            pltpu.VMEM((FFN_LOC, HIDDEN), BF16),
            pltpu.VMEM((4 * ROWS, FFN_LOC), BF16),
            pltpu.VMEM(piece, BF16), pltpu.VMEM(piece, BF16),
            pltpu.VMEM(piece, BF16), pltpu.VMEM(piece, BF16),
            pltpu.VMEM(piece, F32), pltpu.VMEM(piece, BF16), pltpu.VMEM(piece, BF16),
            pltpu.VMEM(piece, F32),
            pltpu.VMEM((2 * ROWS, DIRECT), BF16), pltpu.VMEM((2 * ROWS, DIRECT), BF16),
            dma((2,)), dma((RING + 1,)), dma((N_W,)),
            dma((AG_PIECES,)), dma((AG_PIECES,)), dma, dma, dma((AG_PIECES,)), dma((AG_PIECES,)),
            dma((N_D,)), dma((N_D,)), dma((N_D,)), dma((N_D,)), dma((N_D,)), dma((N_D,)), dma((2,)), dma((2,)),
        ],
        compiler_params=pltpu.CompilerParams(vmem_limit_bytes=50 * 1024 * 1024, collective_id=0, has_side_effects=True),
        name="mlp_block",
    )(m, h, w_in, w_out)


def rope_freq():
    pair = 2 * (np.arange(HEAD_DIM) // 2)
    return jnp.asarray((ROPE_BASE ** (-pair / (HEAD_DIM // 2)))[None, :], F32)


def solution(mesh):
    row_spec = P(('rep', 'grp'))
    repl_spec = P()

    def local_layer(x_in, seq_len, k_cache, v_cache, gamma_attn, w_qkv, b_qkv, w_proj, gamma_mlp, w_in, w_out):
        k_flat = k_cache.reshape(ROWS, FLAT, HEAD_DIM)
        v_flat = v_cache.reshape(ROWS, FLAT, HEAD_DIM)
        h, m, k_out, v_out = attention(seq_len, rope_freq(), x_in, gamma_attn, gamma_mlp, b_qkv, w_qkv, k_flat, v_flat, w_proj)
        layer_out = mlp(m, h, w_in, w_out)
        return layer_out, k_out.reshape(k_cache.shape), v_out.reshape(v_cache.shape)

    return jax.shard_map(local_layer, mesh=mesh,
                         in_specs=(row_spec, row_spec, row_spec, row_spec, repl_spec, repl_spec, repl_spec,
                                   repl_spec, repl_spec, P(None, 'grp', None), P('grp', None)),
                         out_specs=(row_spec, row_spec, row_spec), check_vma=False)
```
